32 devices in a mesh: dp: 1 (over z), sp: 32 (over x, y, core).
Axes of the slice: x: 4, y: 4, z: 1, core: 2. Of those that a mesh axis runs over, the one named last changes fastest.
The devices are a block of a 4x4x8 slice.
Arguments:
- x: bfloat16 [4096, 4096], P(('dp', 'sp'))
- gain: bfloat16 [4096], replicated
- wq: bfloat16 [4096, 4096], replicated
- wk: bfloat16 [4096, 256], replicated
- wv: bfloat16 [4096, 256], replicated
- wo: bfloat16 [4096, 4096], replicated
Outputs:
- output: bfloat16 [4096, 4096], P(('dp', 'sp'))
All inputs are finite; a program needn't handle non-finite values.
Results may differ from the reference program's by a relative error of at most 0.012.
Values are sent between devices in bfloat16 or wider.
A program may use at most 768 MiB of HBM per device.

```python
import jax
import jax.numpy as jnp
from jax import lax

ROWS = 4096
D = 4096
HEADS = 16
KV_HEADS = 1
HEAD = 256
THETA = 10000


def setup_inputs(seed: int = 0, part: int = 0) -> dict:
    kx, kn, kq, kk, kv, ko = jax.random.split(jax.random.key(seed), 6)

    def weights(key, rows, columns):
        return jax.random.normal(key, (rows, columns), jnp.float32) * rows**-0.5

    drawn = {
        "x": jax.random.normal(jax.random.fold_in(kx, part), (ROWS, D), jnp.float32),
        "gain": 1 + 0.1 * jax.random.normal(kn, (D,), jnp.float32),
        "wq": 2 * weights(kq, D, HEADS * HEAD),
        "wk": 2 * weights(kk, D, KV_HEADS * HEAD),
        "wv": 4 * weights(kv, D, KV_HEADS * HEAD),
        "wo": weights(ko, HEADS * HEAD, D),
    }
    return {k: v.astype(jnp.bfloat16) for k, v in drawn.items()}


def normed(x, gain):
    wide = x.astype(jnp.float32)
    scale = lax.rsqrt(jnp.mean(wide * wide, -1, keepdims=True) + 1e-6)
    return (wide * scale * gain.astype(jnp.float32)).astype(jnp.bfloat16)


def turned(t, place, theta):
    half = t.shape[-1] // 2
    angle = place.astype(jnp.float32)[:, None] * theta ** (-jnp.arange(half, dtype=jnp.float32) / half)
    cos, sin = jnp.cos(angle)[:, None], jnp.sin(angle)[:, None]
    a, b = t[..., :half].astype(jnp.float32), t[..., half:].astype(jnp.float32)
    return jnp.concatenate([a * cos - b * sin, b * cos + a * sin], -1).astype(jnp.bfloat16)


def matmul(a, w):
    return jnp.dot(a, w, preferred_element_type=jnp.float32).astype(jnp.bfloat16)


def einsum(form, a, b):
    return jnp.einsum(form, a.astype(jnp.float32), b.astype(jnp.float32))


def attention(q, k, v):
    scores = einsum("tgsd,ugd->gstu", q, k) * q.shape[-1] ** -0.5
    token = jnp.arange(q.shape[0])
    scores = jnp.where(token[:, None] >= token, scores, -jnp.inf)
    weights = jax.nn.softmax(scores, -1).astype(jnp.bfloat16)
    return einsum("gstu,ugd->tgsd", weights, v).astype(jnp.bfloat16)


def reference(x, gain, wq, wk, wv, wo):
    a, place = normed(x, gain), jnp.arange(ROWS)
    q = turned(matmul(a, wq).reshape(ROWS, HEADS, HEAD), place, THETA).reshape(ROWS, KV_HEADS, -1, HEAD)
    k = turned(matmul(a, wk).reshape(ROWS, KV_HEADS, HEAD), place, THETA)
    v = matmul(a, wv).reshape(ROWS, KV_HEADS, HEAD)
    seen = attention(q, k, v).reshape(ROWS, HEADS * HEAD)
    return (x.astype(jnp.float32) + jnp.dot(seen, wo, preferred_element_type=jnp.float32)).astype(jnp.bfloat16)
```

```python
import functools
import math

import jax
import jax.numpy as jnp
import numpy as np
from jax import lax
from jax.experimental import pallas as pl
from jax.experimental.pallas import tpu as pltpu
from jax.sharding import PartitionSpec as P

HEAD = 256
HALF = HEAD // 2
THETA = 10000
EPS = 1e-6
NEG = -1e30
HIDDEN = 2 * NEG
SCALE = HEAD**-0.5
LOG2E = 1.4426950408889634
STRIP = 512
CHUNK = 512
ROWS = 16
F32, BF16 = jnp.float32, jnp.bfloat16


def dot(a, b, ca=1, cb=0):
    return lax.dot_general(a, b, (((ca,), (cb,)), ((), ())), preferred_element_type=F32)


def many(n, f):
    lax.fori_loop(0, n, lambda i, _: (f(i), None)[1], None)


def kernel(n, own, depth, x_h, gain_h, wq_h, wk_h, wv_h, wo_h, rel_h, base_h, out_h,
           x_s, xn_s, gain_s, wk_s, wv_s, wq_s, wo_s, rel_s, base_s, cos_s, sin_s, kv_s, q_s, top_s, mix_s, o_s, acc_s, y_s,
           load_sem, wq_sem, wo_sem, recv_sem, send_sem, x_sem, o_sem, y_sem, out_sem):
    side = math.isqrt(n // 2)
    both = 2 * own
    me = lax.axis_index("sp")
    core, chip = lax.rem(me, 2), lax.div(me, 2)
    row, col = lax.div(chip, side), lax.rem(chip, side)
    mate = me + 1 - 2 * core
    half = depth // 2
    chunks = half // CHUNK
    heads = CHUNK // HEAD

    def device(r, c, k):
        return (r * side + c) * 2 + k

    def along_row(d):
        return lax.rem(col + d, side)

    def load(src, dst, i):
        return pltpu.make_async_copy(src, dst, load_sem.at[i])

    load_x = load(x_h, x_s.at[core], 0)
    load_gain = load(gain_h, gain_s, 1)
    load_wk = load(wk_h, wk_s, 2)
    load_wv = load(wv_h, wv_s, 3)
    load_rel = load(rel_h, rel_s, 4)
    load_base = load(base_h.at[chip], base_s, 5)
    mine = pl.multiple_of(core * half, CHUNK)

    def load_wq(j):
        return pltpu.make_async_copy(wq_h.at[:, pl.ds(pl.multiple_of(mine + j * CHUNK, CHUNK), CHUNK)], wq_s.at[j], wq_sem.at[j])

    def load_wo(j, k):
        return pltpu.make_async_copy(
            wo_h.at[pl.ds(k * half, half), pl.ds(pl.multiple_of(mine + j * CHUNK, CHUNK), CHUNK)], wo_s.at[j, k], wo_sem.at[j, k])

    for c in (load_x, load_gain, load_base, load_rel, load_wk, load_wv):
        c.start()
    for j in range(chunks):
        load_wq(j).start()
    for j in range(chunks):
        for k in range(2):
            load_wo(j, k).start()

    barrier = pltpu.get_barrier_semaphore()
    peers = [mate] + [device(row, along_row(d), core) for d in range(1, side)]
    peers += [device(lax.rem(row + d, side), col, core) for d in range(1, side)]
    for p in peers:
        pl.semaphore_signal(barrier, inc=1, device_id={"sp": p}, device_id_type=pl.DeviceIdType.MESH)
    pl.semaphore_wait(barrier, len(peers))

    def remote(src, dst, send, recv, to):
        return pltpu.make_async_remote_copy(src_ref=src, dst_ref=dst, send_sem=send, recv_sem=recv, device_id={"sp": to},
                                            device_id_type=pl.DeviceIdType.MESH)

    def block(b, to, i):
        return remote(kv_s.at[b], kv_s.at[b], send_sem.at[i], recv_sem.at[b], to)

    def arrived(b):
        block(b, mate, 0).wait_recv()

    give_x = remote(x_s.at[core], x_s.at[core], x_sem.at[0], x_sem.at[1], mate)
    take_x = remote(x_s.at[1 - core], x_s.at[1 - core], x_sem.at[0], x_sem.at[1], mate)

    load_base.wait()
    load_rel.wait()
    bc, bs = base_s[0:1, :], base_s[1:2, :]
    rc, rs = rel_s[0], rel_s[1]
    cos_s[...] = bc * rc - bs * rs
    sin_s[...] = bs * rc + bc * rs
    load_x.wait()
    give_x.start()
    load_gain.wait()

    def norm(h):
        def some(i):
            at = pl.ds(pl.multiple_of(i * ROWS, ROWS), ROWS)
            wide = x_s[h, at, :].astype(F32)
            scale = lax.rsqrt(jnp.mean(wide * wide, -1, keepdims=True) + EPS)
            xn_s[h, at, :] = (wide * scale * gain_s[...].astype(F32)).astype(BF16)

        many(own // ROWS, some)

    def turned(t, cos, sin):
        a, b = t[:, :HALF].astype(F32), t[:, HALF:].astype(F32)
        return (a * cos - b * sin).astype(BF16), (b * cos + a * sin).astype(BF16)

    norm(core)
    at = pl.ds(pl.multiple_of(core * own, own), own)
    load_wk.wait()
    ka, kb = turned(dot(xn_s[core], wk_s[...]).astype(BF16), cos_s[at, :], sin_s[at, :])
    kv_s[me, 0] = ka
    kv_s[me, 1] = kb
    load_wv.wait()
    v = dot(xn_s[core], wv_s[...]).astype(BF16).T
    kv_s[me, 2] = v[:HALF]
    kv_s[me, 3] = v[HALF:]

    down = range(side - 1, 0, -1)
    SECOND = 2 * side - 1
    THIRD = SECOND + (side - 1) * side

    def to_row(b, i, act):
        for d in range(1, side):
            act(block(b, device(row, along_row(d), core), i + d - 1))

    def to_rows(b, i, act):
        for d in down:
            @pl.when(row + d < side)
            def _():
                act(block(b, device(row + d, col, core), i + d - 1))

    def first(act):
        @pl.when(core == 0)
        def _():
            to_row(me, 0, act)
            to_rows(me, side - 1, act)

        @pl.when(core == 1)
        def _():
            to_rows(me, side - 1, act)
            to_row(me, 0, act)

        act(block(me, mate, 2 * side - 2))

    def second(i, act, wait):
        at = SECOND + (i - 1) * side

        @pl.when(core == 0)
        def _():
            b = device(row, along_row(side - i), 0)
            if wait:
                arrived(b)
            to_rows(b, at, act)
            act(block(b, mate, at + side - 1))

        @pl.when((core == 1) & (row >= i))
        def _():
            b = device(row - i, col, 1)
            if wait:
                arrived(b)
            to_row(b, at, act)
            act(block(b, mate, at + side - 1))

    def third(t, act, wait):
        at = THIRD + t * side

        @pl.when((core == 0) & (t > 0))
        def _():
            for c in range(side):
                b = device(row - t, c, 0)
                if wait:
                    arrived(b)
                act(block(b, mate, at + c))

        @pl.when(core == 1)
        def _():
            for d in range(1, side):
                b = device(row - t, along_row(d), 1)
                if wait:
                    arrived(b)
                act(block(b, mate, at + d))

    start = lambda c: c.start()
    sent = lambda c: c.wait_send()
    first(start)

    take_x.wait_recv()
    norm(1 - core)

    def make_queries(j):
        load_wq(j).wait()
        q = dot(xn_s[...].reshape(both, depth), wq_s[j]).astype(BF16)
        for h in range(heads):
            a, b = turned(q[:, h * HEAD : (h + 1) * HEAD], cos_s[...], sin_s[...])
            q_s[j, :HALF, h * both : (h + 1) * both] = a.T
            q_s[j, HALF:, h * both : (h + 1) * both] = b.T

        @pl.when(j > 0)
        def _():
            second(j, start, True)

    many(chunks, make_queries)

    strips = range(chunks)
    wide = heads * both
    e = SCALE * LOG2E
    for s in strips:
        top_s[s] = jnp.full((1, wide), NEG, F32)
        mix_s[s] = jnp.zeros((HEAD + 8, wide), F32)
    ones = jnp.ones((8, side * own), BF16)

    def attend(r, kind, masked):
        blocks = [device(r, c, kind) for c in range(side)]
        keys = jnp.concatenate([jnp.concatenate([kv_s[b, 0], kv_s[b, 1]], axis=1) for b in blocks], axis=0)
        values = jnp.concatenate([jnp.concatenate([kv_s[b, 2], kv_s[b, 3]], axis=0) for b in blocks], axis=1)
        values = jnp.concatenate([values, ones], axis=0)
        scores = [dot(keys, q_s[s]) for s in strips]
        if masked:
            gap = lax.broadcasted_iota(jnp.int32, (own, both), 1) - lax.broadcasted_iota(jnp.int32, (own, both), 0)
            ok = jnp.concatenate([gap >= b * own - chip * both for b in blocks], axis=0)
            ok = jnp.concatenate([ok] * heads, axis=1)
            scores = [jnp.where(ok, s, HIDDEN) for s in scores]
        weights, keeps = [], []
        for s in strips:
            old = top_s[s]
            top = jnp.maximum(old, scores[s].max(axis=0, keepdims=True))
            top_s[s] = top
            weights.append(jnp.exp2((scores[s] - top) * e).astype(BF16))
            keeps.append(jnp.exp2((old - top) * e))
        for s in strips:
            mix_s[s] = mix_s[s] * keeps[s] + dot(values, weights[s])

    def other(r):
        for c in range(side):
            arrived(device(r, c, 1 - core))

    third(0, start, True)
    other(row)
    many(2, lambda k: attend(row, k, True))

    def later(t):
        third(t + 1, start, True)
        attend(row - 1 - t, core, False)
        other(row - 1 - t)
        attend(row - 1 - t, 1 - core, False)

    many(row, later)

    def give_o(s):
        at = pl.ds(pl.multiple_of(s * CHUNK, CHUNK), CHUNK)
        return remote(o_s.at[core, :, at], o_s.at[core, :, at], o_sem.at[0, s], o_sem.at[1, s], mate)

    def finish(s):
        whole = mix_s[s, :HEAD, :] * (1 / mix_s[s, HEAD : HEAD + 1, :])
        for h in range(heads):
            o_s[core, :, pl.ds(pl.multiple_of(s * CHUNK + h * HEAD, HEAD), HEAD)] = whole[:, h * both : (h + 1) * both].T.astype(BF16)
        give_o(s).start()

    many(chunks, finish)

    def own_part(j):
        load_wo(j, core).wait()
        acc_s[j] = dot(o_s[core], wo_s[j, core])

    many(chunks, own_part)
    for s in strips:
        at = pl.ds(s * CHUNK, CHUNK)
        remote(o_s.at[1 - core, :, at], o_s.at[1 - core, :, at], o_sem.at[0, s], o_sem.at[1, s], mate).wait_recv()

    def give_y(j, there):
        at = pl.ds(pl.multiple_of(there * half + j * CHUNK, CHUNK), CHUNK)
        return remote(y_s.at[j, 1 - core], out_h.at[:, at], y_sem.at[0, j], y_sem.at[1, j], mate)

    def keep_y(j):
        at = pl.ds(pl.multiple_of(mine + j * CHUNK, CHUNK), CHUNK)
        return pltpu.make_async_copy(y_s.at[j, core], out_h.at[:, at], out_sem.at[j])

    def rest(j):
        load_wo(j, 1 - core).wait()
        at = pl.ds(pl.multiple_of(mine + j * CHUNK, CHUNK), CHUNK)
        whole = acc_s[j] + dot(o_s[1 - core], wo_s[j, 1 - core])
        for h in range(2):
            y_s[j, h] = (x_s[h, :, at].astype(F32) + whole[h * own : (h + 1) * own]).astype(BF16)
        give_y(j, core).start()
        keep_y(j).start()

    many(chunks, rest)

    give_x.wait_send()
    first(sent)
    for i in range(1, side):
        second(i, sent, False)
    third(0, sent, False)
    many(row, lambda t: third(t + 1, sent, False))
    for j in range(chunks):
        give_o(j).wait_send()
        give_y(j, core).wait_send()
        keep_y(j).wait()
        give_y(j, 1 - core).wait_recv()


def angles(places):
    freq = THETA ** (-np.arange(HALF, dtype=np.float64) / HALF)
    a = np.asarray(places, np.float64)[:, None] * freq
    return np.stack([np.cos(a), np.sin(a)]).astype(np.float32)


def solution(mesh):
    n = mesh.shape["sp"]

    def step(x, gain, wq, wk, wv, wo):
        own, depth = x.shape
        both, half = 2 * own, depth // 2
        chunks = half // CHUNK
        wide = CHUNK // HEAD * both
        side = math.isqrt(n // 2)
        rel = angles(np.arange(both))
        base = angles(np.arange(n // 2) * both).transpose(1, 0, 2)
        base = np.pad(base, ((0, 0), (0, 6), (0, 0)))
        dma = pltpu.SemaphoreType.DMA
        hbm = pl.BlockSpec(memory_space=pltpu.HBM)
        return pl.pallas_call(
            functools.partial(kernel, n, own, depth),
            out_shape=jax.ShapeDtypeStruct(x.shape, x.dtype),
            in_specs=[hbm] * 8,
            out_specs=hbm,
            scratch_shapes=[
                pltpu.VMEM((2, own, depth), BF16),
                pltpu.VMEM((2, own, depth), BF16),
                pltpu.VMEM((1, depth), BF16),
                pltpu.VMEM((depth, HEAD), BF16),
                pltpu.VMEM((depth, HEAD), BF16),
                pltpu.VMEM((chunks, depth, CHUNK), BF16),
                pltpu.VMEM((chunks, 2, half, CHUNK), BF16),
                pltpu.VMEM((2, both, HALF), F32),
                pltpu.VMEM((8, HALF), F32),
                pltpu.VMEM((both, HALF), F32),
                pltpu.VMEM((both, HALF), F32),
                pltpu.VMEM((n, 4, own, HALF), BF16),
                pltpu.VMEM((chunks, HEAD, wide), BF16),
                pltpu.VMEM((chunks, 1, wide), F32),
                pltpu.VMEM((chunks, HEAD + 8, wide), F32),
                pltpu.VMEM((2, both, half), BF16),
                pltpu.VMEM((chunks, both, CHUNK), F32),
                pltpu.VMEM((chunks, 2, own, CHUNK), BF16),
                dma((6,)),
                dma((chunks,)),
                dma((chunks, 2)),
                dma((n,)),
                dma((2 * side - 1 + (side - 1) * side + side * side,)),
                dma((2,)),
                dma((2, chunks)),
                dma((2, chunks)),
                dma((chunks,)),
            ],
            compiler_params=pltpu.CompilerParams(collective_id=0, has_side_effects=True, vmem_limit_bytes=67043328),
        )(x, gain[None], wq, wk, wv, wo, jnp.asarray(rel), jnp.asarray(base))

    tokens, whole = P(("dp", "sp"), None), P(None, None)
    return jax.shard_map(
        step,
        mesh=mesh,
        in_specs=(tokens, P(None), whole, whole, whole, whole),
        out_specs=tokens,
        check_vma=False,
    )
```

```python
import functools
import math

import jax
import jax.numpy as jnp
import numpy as np
from jax import lax
from jax.experimental import pallas as pl
from jax.experimental.pallas import tpu as pltpu
from jax.sharding import PartitionSpec as P

HEAD = 256
HALF = HEAD // 2
THETA = 10000
EPS = 1e-6
NEG = -1e30
HIDDEN = 2 * NEG
SCALE = HEAD**-0.5
LOG2E = 1.4426950408889634
AHEAD = 1
VMEM = 62 * 2**20
CHUNK = 512
ROWS = 16
F32, BF16 = jnp.float32, jnp.bfloat16


def dot(a, b, ca=1, cb=0):
    return lax.dot_general(a, b, (((ca,), (cb,)), ((), ())), preferred_element_type=F32)


def scope(name, f):
    with jax.named_scope(name):
        return f()


def many(n, f, unroll=1):
    lax.fori_loop(0, n, lambda i, _: (f(i), None)[1], None, unroll=unroll)


def kernel(n, own, depth, x_h, gain_h, wq_h, wk_h, wv_h, wo_h, rel_h, base_h, out_ref,
           x_s, xn_s, gain_s, wk_s, wv_s, wq_s, wo_s, rel_s, base_s, cos_s, sin_s, kv_s, q_s, top_s, mix_s, o_s, acc_s, y_s,
           load_sem, wq_sem, wo_sem, recv_sem, send_sem, x_sem, o_sem, y_sem, meet, go):
    side = math.isqrt(n // 2)
    both = 2 * own
    me = lax.axis_index("sp")
    core, chip = lax.rem(me, 2), lax.div(me, 2)
    row, col = lax.div(chip, side), lax.rem(chip, side)
    mate = me + 1 - 2 * core
    half = depth // 2
    chunks = half // CHUNK
    per = CHUNK // HEAD
    heads = half // HEAD

    def device(r, c, k):
        return (r * side + c) * 2 + k

    def along_row(d):
        return lax.rem(col + d, side)

    def load(src, dst, i):
        return pltpu.make_async_copy(src, dst, load_sem.at[i])

    load_x = load(x_h, x_s.at[core], 0)
    load_gain = load(gain_h, gain_s, 1)
    load_wk = load(wk_h, wk_s, 2)
    load_wv = load(wv_h, wv_s, 3)
    load_rel = load(rel_h, rel_s, 4)
    load_base = load(base_h.at[chip], base_s, 5)
    mine = pl.multiple_of(core * half, CHUNK)

    def load_wq(j):
        return pltpu.make_async_copy(wq_h.at[:, pl.ds(pl.multiple_of(mine + j * CHUNK, CHUNK), CHUNK)], wq_s.at[j], wq_sem.at[j])

    def load_wo(j, k):
        return pltpu.make_async_copy(
            wo_h.at[pl.ds(k * half, half), pl.ds(pl.multiple_of(mine + j * CHUNK, CHUNK), CHUNK)], wo_s.at[j, k], wo_sem.at[j, k])

    for c in (load_x, load_gain, load_base, load_rel, load_wk, load_wv):
        c.start()
    load_wq(0).start()

    barrier = pltpu.get_barrier_semaphore()
    peers = [device(row, along_row(d), 1) for d in range(1, side)] + [device(lax.rem(row + d, side), col, 1) for d in range(1, side)]

    def tell(sem, to):
        pl.semaphore_signal(sem, inc=1, device_id={"sp": to}, device_id_type=pl.DeviceIdType.MESH)

    def greet():
        @pl.when(core == 1)
        def _():
            tell(barrier, mate)

        @pl.when(core == 0)
        def _():
            pl.semaphore_wait(barrier, 1)
            tell(meet, mate)

        @pl.when(core == 1)
        def _():
            pl.semaphore_wait(meet, 1)
            for p in peers:
                tell(barrier, p)

    def gather():
        @pl.when(core == 1)
        def _():
            pl.semaphore_wait(barrier, len(peers))
            tell(go, mate)

        @pl.when(core == 0)
        def _():
            pl.semaphore_wait(go, 1)

    scope("greet", greet)

    def remote(src, dst, send, recv, to):
        return pltpu.make_async_remote_copy(src_ref=src, dst_ref=dst, send_sem=send, recv_sem=recv, device_id={"sp": to},
                                            device_id_type=pl.DeviceIdType.MESH)

    def block(b, to, i):
        return remote(kv_s.at[b], kv_s.at[b], send_sem.at[i], recv_sem.at[b], to)

    def arrived(b):
        block(b, mate, 0).wait_recv()

    give_x = remote(x_s.at[core], x_s.at[core], x_sem.at[0], x_sem.at[1], mate)
    take_x = remote(x_s.at[1 - core], x_s.at[1 - core], x_sem.at[0], x_sem.at[1], mate)

    load_base.wait()
    load_rel.wait()
    bc, bs = base_s[0:1, :], base_s[1:2, :]
    rc, rs = rel_s[0], rel_s[1]
    cos_s[...] = bc * rc - bs * rs
    sin_s[...] = bs * rc + bc * rs
    scope("x_wait", load_x.wait)
    give_x.start()
    load_gain.wait()

    gain = gain_s[...].astype(F32).reshape(1, depth)

    def norm(h):
        def some(i):
            at = pl.ds(pl.multiple_of(i * ROWS, ROWS), ROWS)
            wide = x_s[h, at, :].astype(F32)
            scale = lax.rsqrt(jnp.mean(wide * wide, -1, keepdims=True) + EPS)
            xn_s[h, at, :] = (wide * scale * gain).astype(BF16)

        many(own // ROWS, some, 4)

    def turned(t, cos, sin):
        a, b = t[:, :HALF].astype(F32), t[:, HALF:].astype(F32)
        return (a * cos - b * sin).astype(BF16), (b * cos + a * sin).astype(BF16)

    for j in range(1, chunks):
        load_wq(j).start()
    scope("norm_own", lambda: norm(core))
    at = pl.ds(pl.multiple_of(core * own, own), own)
    scope("wk_wait", load_wk.wait)
    load_wv.wait()
    ka, kb = turned(dot(xn_s[core], wk_s[...]).astype(BF16), cos_s[at, :], sin_s[at, :])
    kv_s[me, 0] = ka
    kv_s[me, 1] = kb
    v = dot(xn_s[core], wv_s[...]).astype(BF16).T
    kv_s[me, 2] = v[:HALF]
    kv_s[me, 3] = v[HALF:]

    down = range(side - 1, 0, -1)
    SECOND = 2 * side - 1
    THIRD = SECOND + (side - 1) * side
    last = row == side - 1

    def to_row(b, i, act, needs=None):
        for d in range(1, side):
            to = along_row(d)
            if needs is None:
                act(block(b, device(row, to, core), i + d - 1))
            else:
                @pl.when(needs(to))
                def _():
                    act(block(b, device(row, to, core), i + d - 1))

    def to_rows(b, i, act):
        for d in down:
            @pl.when(row + d < side)
            def _():
                act(block(b, device(row + d, col, core), i + d - 1))

    def first(act):
        @pl.when(core == 0)
        def _():
            to_row(me, 0, act, lambda c: jnp.logical_not(last) | (c > col))
            to_rows(me, side - 1, act)

        @pl.when(core == 1)
        def _():
            to_rows(me, side - 1, act)
            to_row(me, 0, act, lambda c: c > col)

        act(block(me, mate, 2 * side - 2))

    def second(i, act, wait):
        at = SECOND + (i - 1) * side
        c = along_row(side - i)

        @pl.when((core == 0) & (jnp.logical_not(last) | (c < col)))
        def _():
            b = device(row, c, 0)
            if wait:
                arrived(b)
            to_rows(b, at, act)

            @pl.when(c < col)
            def _():
                act(block(b, mate, at + side - 1))

        @pl.when((core == 1) & (row >= i))
        def _():
            b = device(row - i, col, 1)
            if wait:
                arrived(b)
            to_row(b, at, act)
            act(block(b, mate, at + side - 1))

    def beside(c, act, wait):
        @pl.when((core == 1) & (c >= 0))
        def _():
            b = device(row, c, 1)
            if wait:
                arrived(b)
            act(block(b, mate, THIRD + c))

    def third(t, act, wait):
        at = THIRD + t * side

        @pl.when(core == 0)
        def _():
            for c in range(side):
                b = device(row - t, c, 0)
                if wait:
                    arrived(b)
                act(block(b, mate, at + c))

        @pl.when(core == 1)
        def _():
            for d in range(1, side):
                b = device(row - t, along_row(d), 1)
                if wait:
                    arrived(b)
                act(block(b, mate, at + d))

    start = lambda c: c.start()
    sent = lambda c: c.wait_send()
    scope("gather", gather)
    scope("first", lambda: first(start))

    scope("x_take", take_x.wait_recv)
    scope("norm_mate", lambda: norm(1 - core))

    def make_queries(j):
        scope("wq_wait", load_wq(j).wait)
        q = dot(xn_s[...].reshape(both, depth), wq_s[j]).astype(BF16)
        for h in range(per):
            a, b = turned(q[:, h * HEAD : (h + 1) * HEAD], cos_s[...], sin_s[...])
            q_s[j * per + h, :HALF] = a.T
            q_s[j * per + h, HALF:] = b.T

    for j in range(chunks):
        for k in range(2):
            load_wo(j, k).start()
    scope("queries", lambda: many(chunks, make_queries))

    def pass_on():
        for i in (1, *range(side - 1, 1, -1)):
            second(i, start, True)

    scope("second", pass_on)

    e = SCALE * LOG2E
    for h in range(heads):
        top_s[h] = jnp.full((1, both), NEG, F32)
        mix_s[h] = jnp.zeros((HEAD + 8, both), F32)

    def attend(blocks, masked=False):
        keys = jnp.concatenate([jnp.concatenate([kv_s[b, 0], kv_s[b, 1]], axis=1) for b in blocks], axis=0)
        values = jnp.concatenate([jnp.concatenate([kv_s[b, 2], kv_s[b, 3]], axis=0) for b in blocks], axis=1)
        values = jnp.concatenate([values, jnp.ones((8, values.shape[1]), BF16)], axis=0)
        if masked:
            ok = lax.broadcasted_iota(jnp.int32, (both, both), 1) >= lax.broadcasted_iota(jnp.int32, (both, both), 0)

        def mix(h, s):
            if masked:
                s = jnp.where(ok, s, HIDDEN)
            old = top_s[h]
            top = jnp.maximum(old, s.max(axis=0, keepdims=True))
            top_s[h] = top
            weights = jnp.exp2((s - top) * e).astype(BF16)
            mix_s[h] = mix_s[h] * jnp.exp2((old - top) * e) + dot(values, weights)

        ahead = []
        for h in range(heads):
            ahead.append((h, dot(keys, q_s[h])))
            if len(ahead) > AHEAD:
                mix(*ahead.pop(0))
        for a in ahead:
            mix(*a)

    def chip_blocks(r, c):
        return [device(r, c, 0), device(r, c, 1)]

    def row_blocks(r, k):
        return [device(r, c, k) for c in range(side)]

    def wait_mate(blocks):
        for b in blocks:
            arrived(b)

    scope("beside", lambda: beside(col - 1, start, True))
    scope("mate", lambda: arrived(mate))
    scope("diagonal", lambda: attend(chip_blocks(row, col), True))

    def own_row(t):
        c = col - 1 - t
        scope("beside", lambda: beside(c - 1, start, True))
        scope("other", lambda: arrived(device(row, c, 1 - core)))
        scope("near", lambda: attend(chip_blocks(row, c)))

    many(col, own_row)

    def earlier_row(t):
        r = row - 1 - t
        scope("third", lambda: third(t + 1, start, True))
        scope("attend", lambda: attend(row_blocks(r, core)))
        scope("other", lambda: wait_mate(row_blocks(r, 1 - core)))
        scope("attend", lambda: attend(row_blocks(r, 1 - core)))

    many(row, earlier_row)

    def give_o(s):
        at = pl.ds(pl.multiple_of(s * CHUNK, CHUNK), CHUNK)
        return remote(o_s.at[core, :, at], o_s.at[core, :, at], o_sem.at[0, s], o_sem.at[1, s], mate)

    def finish(s):
        for h in range(per):
            i = s * per + h
            whole = mix_s[i, :HEAD, :] * (1 / mix_s[i, HEAD : HEAD + 1, :])
            o_s[core, :, pl.ds(pl.multiple_of(s * CHUNK + h * HEAD, HEAD), HEAD)] = whole.T.astype(BF16)
        give_o(s).start()

    scope("finish", lambda: many(chunks, finish))

    for j in range(chunks):
        for k in range(2):
            load_wo(j, k).wait()

    def own_part(j):
        acc_s[j] = dot(o_s[core], wo_s[j, core])

    def take_o():
        for s in range(chunks):
            at = pl.ds(s * CHUNK, CHUNK)
            remote(o_s.at[1 - core, :, at], o_s.at[1 - core, :, at], o_sem.at[0, s], o_sem.at[1, s], mate).wait_recv()

    scope("own_part", lambda: many(chunks, own_part, chunks))
    scope("o_take", take_o)

    def give_y(j, there):
        at = pl.ds(pl.multiple_of(there * half + j * CHUNK, CHUNK), CHUNK)
        return remote(y_s.at[j], out_ref.at[:, at], y_sem.at[0, j], y_sem.at[1, j], mate)

    def rest(j):
        at = pl.ds(pl.multiple_of(mine + j * CHUNK, CHUNK), CHUNK)
        acc_s[j] = acc_s[j] + dot(o_s[1 - core], wo_s[j, 1 - core])
        y_s[j] = (x_s[1 - core, :, at].astype(F32) + acc_s[j, pl.ds(pl.multiple_of((1 - core) * own, own), own), :]).astype(BF16)
        give_y(j, core).start()
        out_ref[:, at] = (x_s[core, :, at].astype(F32) + acc_s[j, pl.ds(pl.multiple_of(core * own, own), own), :]).astype(BF16)

    scope("rest", lambda: many(chunks, rest))

    ending = jax.named_scope("ending")
    ending.__enter__()
    give_x.wait_send()
    first(sent)
    for i in range(1, side):
        second(i, sent, False)
    many(col, lambda t: beside(t, sent, False))
    many(row, lambda t: third(t + 1, sent, False))
    for j in range(chunks):
        give_o(j).wait_send()
        give_y(j, core).wait_send()
        give_y(j, 1 - core).wait_recv()
    ending.__exit__(None, None, None)


def angles(places):
    freq = THETA ** (-np.arange(HALF, dtype=np.float64) / HALF)
    a = np.asarray(places, np.float64)[:, None] * freq
    return np.stack([np.cos(a), np.sin(a)]).astype(np.float32)


def solution(mesh):
    n = mesh.shape["sp"]

    def step(x, gain, wq, wk, wv, wo):
        own, depth = x.shape
        both, half = 2 * own, depth // 2
        chunks = half // CHUNK
        heads = half // HEAD
        side = math.isqrt(n // 2)
        rel = angles(np.arange(both))
        base = angles(np.arange(n // 2) * both).transpose(1, 0, 2)
        base = np.pad(base, ((0, 0), (0, 6), (0, 0)))
        dma = pltpu.SemaphoreType.DMA
        hbm = pl.BlockSpec(memory_space=pltpu.HBM)
        return pl.pallas_call(
            functools.partial(kernel, n, own, depth),
            out_shape=pltpu.VMEM(x.shape, x.dtype),
            in_specs=[hbm] * 8,
            out_specs=pl.BlockSpec(memory_space=pltpu.VMEM),
            scratch_shapes=[
                pltpu.VMEM((2, own, depth), BF16),
                pltpu.VMEM((2, own, depth), BF16),
                pltpu.VMEM((depth,), BF16),
                pltpu.VMEM((depth, HEAD), BF16),
                pltpu.VMEM((depth, HEAD), BF16),
                pltpu.VMEM((chunks, depth, CHUNK), BF16),
                pltpu.VMEM((chunks, 2, half, CHUNK), BF16),
                pltpu.VMEM((2, both, HALF), F32),
                pltpu.VMEM((8, HALF), F32),
                pltpu.VMEM((both, HALF), F32),
                pltpu.VMEM((both, HALF), F32),
                pltpu.VMEM((n, 4, own, HALF), BF16),
                pltpu.VMEM((heads, HEAD, both), BF16),
                pltpu.VMEM((heads, 1, both), F32),
                pltpu.VMEM((heads, HEAD + 8, both), F32),
                pltpu.VMEM((2, both, half), BF16),
                pltpu.VMEM((chunks, both, CHUNK), F32),
                pltpu.VMEM((chunks, own, CHUNK), BF16),
                dma((6,)),
                dma((chunks,)),
                dma((chunks, 2)),
                dma((n,)),
                dma((2 * side - 1 + (side - 1) * side + side * side,)),
                dma((2,)),
                dma((2, chunks)),
                dma((2, chunks)),
                pltpu.SemaphoreType.REGULAR,
                pltpu.SemaphoreType.REGULAR,
            ],
            compiler_params=pltpu.CompilerParams(collective_id=0, has_side_effects=True, vmem_limit_bytes=VMEM),
        )(x, gain, wq, wk, wv, wo, jnp.asarray(rel), jnp.asarray(base))

    tokens, whole = P(("dp", "sp"), None), P(None, None)
    return jax.shard_map(
        step,
        mesh=mesh,
        in_specs=(tokens, P(None), whole, whole, whole, whole),
        out_specs=tokens,
        check_vma=False,
    )
```

```python
import functools
import math

import jax
import jax.numpy as jnp
import numpy as np
from jax import lax
from jax.experimental import pallas as pl
from jax.experimental.pallas import tpu as pltpu
from jax.sharding import PartitionSpec as P

HEAD = 256
HALF = HEAD // 2
THETA = 10000
EPS = 1e-6
NEG = -1e30
HIDDEN = 2 * NEG
SCALE = HEAD**-0.5
LOG2E = 1.4426950408889634
AHEAD = 7
BEHIND = 7
VMEM = 62 * 2**20
PASS = 1, 2
CHUNK = 512
ROWS = 16
F32, BF16 = jnp.float32, jnp.bfloat16


def dot(a, b, ca=1, cb=0):
    return lax.dot_general(a, b, (((ca,), (cb,)), ((), ())), preferred_element_type=F32)


def scope(name, f):
    with jax.named_scope(name):
        return f()


def many(n, f, unroll=1):
    lax.fori_loop(0, n, lambda i, _: (f(i), None)[1], None, unroll=unroll)


def kernel(n, own, depth, x_h, gain_h, wq_h, wk_h, wv_h, wo_h, rel_h, base_h, out_ref,
           x_s, xn_s, gain_s, wk_s, wv_s, wq_s, wo_s, rel_s, base_s, cos_s, sin_s, kv_s, raw_s, q_s, top_s, mix_s, o_s, acc_s, y_s,
           load_sem, wq_sem, wo_sem, recv_sem, send_sem, x_sem, o_sem, y_sem, meet, go):
    side = math.isqrt(n // 2)
    both = 2 * own
    me = lax.axis_index("sp")
    core, chip = lax.rem(me, 2), lax.div(me, 2)
    row, col = lax.div(chip, side), lax.rem(chip, side)
    mate = me + 1 - 2 * core
    half = depth // 2
    chunks = half // CHUNK
    per = CHUNK // HEAD
    heads = half // HEAD

    def device(r, c, k):
        return (r * side + c) * 2 + k

    def along_row(d):
        return lax.rem(col + d, side)

    def load(src, dst, i):
        return pltpu.make_async_copy(src, dst, load_sem.at[i])

    load_x = load(x_h, x_s.at[core], 0)
    load_gain = load(gain_h, gain_s, 1)
    load_wk = load(wk_h, wk_s, 2)
    load_wv = load(wv_h, wv_s, 3)
    load_rel = load(rel_h, rel_s, 4)
    load_base = load(base_h.at[chip], base_s, 5)
    mine = pl.multiple_of(core * half, CHUNK)

    def load_wq(j):
        return pltpu.make_async_copy(wq_h.at[:, pl.ds(pl.multiple_of(mine + j * CHUNK, CHUNK), CHUNK)], wq_s.at[j], wq_sem.at[j])

    def load_wo(j, k):
        return pltpu.make_async_copy(
            wo_h.at[pl.ds(k * half, half), pl.ds(pl.multiple_of(mine + j * CHUNK, CHUNK), CHUNK)], wo_s.at[j, k], wo_sem.at[j, k])

    for c in (load_x, load_gain, load_base, load_rel, load_wk, load_wv):
        c.start()

    barrier = pltpu.get_barrier_semaphore()
    peers = [device(row, along_row(d), 1) for d in range(1, side)] + [device(lax.rem(row + d, side), col, 1) for d in range(1, side)]

    def tell(sem, to):
        pl.semaphore_signal(sem, inc=1, device_id={"sp": to}, device_id_type=pl.DeviceIdType.MESH)

    def greet():
        @pl.when(core == 1)
        def _():
            tell(barrier, mate)

        @pl.when(core == 0)
        def _():
            pl.semaphore_wait(barrier, 1)
            tell(meet, mate)

        @pl.when(core == 1)
        def _():
            pl.semaphore_wait(meet, 1)
            for p in peers:
                tell(barrier, p)

    def gather():
        @pl.when(core == 1)
        def _():
            pl.semaphore_wait(barrier, len(peers))
            tell(go, mate)

        @pl.when(core == 0)
        def _():
            pl.semaphore_wait(go, 1)

    scope("greet", greet)

    def remote(src, dst, send, recv, to):
        return pltpu.make_async_remote_copy(src_ref=src, dst_ref=dst, send_sem=send, recv_sem=recv, device_id={"sp": to},
                                            device_id_type=pl.DeviceIdType.MESH)

    def block(b, to, i):
        return remote(kv_s.at[b], kv_s.at[b], send_sem.at[i], recv_sem.at[b], to)

    def arrived(b):
        block(b, mate, 0).wait_recv()

    give_x = remote(x_s.at[core], x_s.at[core], x_sem.at[0], x_sem.at[1], mate)
    take_x = remote(x_s.at[1 - core], x_s.at[1 - core], x_sem.at[0], x_sem.at[1], mate)

    load_base.wait()
    load_rel.wait()
    bc, bs = base_s[0:1, :], base_s[1:2, :]
    rc, rs = rel_s[0], rel_s[1]
    cos_s[...] = bc * rc - bs * rs
    sin_s[...] = bs * rc + bc * rs
    scope("x_wait", load_x.wait)
    give_x.start()
    load_gain.wait()

    gain = gain_s[...].astype(F32).reshape(1, depth)

    def norm(h):
        def some(i):
            at = pl.ds(pl.multiple_of(i * ROWS, ROWS), ROWS)
            wide = x_s[h, at, :].astype(F32)
            scale = lax.rsqrt(jnp.mean(wide * wide, -1, keepdims=True) + EPS)
            xn_s[h, at, :] = (wide * scale * gain).astype(BF16)

        many(own // ROWS, some, 4)

    def turned(t, cos, sin):
        a, b = t[:, :HALF].astype(F32), t[:, HALF:].astype(F32)
        return (a * cos - b * sin).astype(BF16), (b * cos + a * sin).astype(BF16)

    scope("norm_own", lambda: norm(core))
    for j in range(chunks):
        load_wq(j).start()
    at = pl.ds(pl.multiple_of(core * own, own), own)
    scope("wk_wait", load_wk.wait)
    ka, kb = turned(dot(xn_s[core], wk_s[...]).astype(BF16), cos_s[at, :], sin_s[at, :])
    kv_s[me, 0] = ka
    kv_s[me, 1] = kb
    scope("wv_wait", load_wv.wait)
    v = dot(xn_s[core], wv_s[...]).astype(BF16).T
    kv_s[me, 2] = v[:HALF]
    kv_s[me, 3] = v[HALF:]

    SECOND = 2 * side - 1
    THIRD = SECOND + side * side
    last = row == side - 1
    near = [1, side - 1, *range(2, side - 1)]

    def to_row(b, i, act, needs=None):
        for d in near:
            to = along_row(d)
            if needs is None:
                act(block(b, device(row, to, core), i + d - 1))
            else:
                @pl.when(needs(to))
                def _():
                    act(block(b, device(row, to, core), i + d - 1))

    def to_column(b, i, act):
        for d in (*range(2, side - 1), side - 1, 1):
            @pl.when(row + d < side)
            def _():
                act(block(b, device(row + d, col, core), i + d - 1))

    def first(act):
        @pl.when(core == 0)
        def _():
            to_row(me, 0, act, lambda c: jnp.logical_not(last) | (c > col))

        to_column(me, side - 1, act)
        act(block(me, mate, 2 * side - 2))

    def own_later(act, now):
        @pl.when((core == 1) & now)
        def _():
            to_row(me, 0, act, lambda c: c > col)

    def second_0(act, wait, now):
        for c in range(side):
            @pl.when((core == 0) & now & (c != col) & (jnp.logical_not(last) | (c < col)))
            def _():
                b, at = device(row, c, 0), SECOND + c * side
                if wait:
                    arrived(b)
                to_column(b, at, act)

                @pl.when(c < col)
                def _():
                    act(block(b, mate, at + side - 1))

    def second_1(act, wait):
        for t in range(side - 1):
            @pl.when((core == 1) & (t < row))
            def _():
                r = earlier(t)
                b, at = device(r, col, 1), SECOND + r * side
                if wait:
                    arrived(b)
                to_row(b, at, act)
                act(block(b, mate, at + side - 1))

    def beside(c, act, wait):
        @pl.when((core == 1) & (c >= 0))
        def _():
            b = device(row, c, 1)
            if wait:
                arrived(b)
            act(block(b, mate, THIRD + c))

    def above(t, act, wait):
        @pl.when((core == 0) & (t < row))
        def _():
            b = device(earlier(t), col, 0)
            if wait:
                arrived(b)
            act(block(b, mate, THIRD + (earlier(t) + 1) * side))

    def earlier(t):
        return jnp.where(last, row - 1 - t, t)

    def third(r, act, wait):
        at = THIRD + (r + 1) * side

        for d in near:
            b = device(r, along_row(d), core)
            if wait:
                arrived(b)

            act(block(b, mate, at + d))

    start = lambda c: c.start()
    sent = lambda c: c.wait_send()
    scope("gather", gather)
    scope("first", lambda: first(start))
    own_later(start, last)

    scope("x_take", take_x.wait_recv)
    scope("norm_mate", lambda: norm(1 - core))

    def turn(j):
        for h in range(per):
            a, b = turned(raw_s[j % 2, :, h * HEAD : (h + 1) * HEAD], cos_s[...], sin_s[...])
            q_s[j * per + h, :HALF] = a.T
            q_s[j * per + h, HALF:] = b.T

    for j in range(chunks):
        for k in range(2):
            load_wo(j, k).start()
    for j in range(chunks):
        scope("wq_wait", load_wq(j).wait)
        with jax.named_scope("queries"):
            raw_s[j % 2] = dot(xn_s[...].reshape(both, depth), wq_s[j]).astype(BF16)
            if j:
                turn(j - 1)
        if j == 0:
            own_later(start, jnp.logical_not(last))
        if j == PASS[0]:
            scope("second", lambda: second_0(start, True, jnp.logical_not(last)))
        if j == PASS[1]:
            scope("second", lambda: second_1(start, True))
    scope("turn", lambda: turn(chunks - 1))

    e = SCALE * LOG2E
    for h in range(heads):
        top_s[h] = jnp.full((1, both), NEG, F32)
        mix_s[h] = jnp.zeros((HEAD + 8, both), F32)

    def attend(blocks, masked=False):
        keys = jnp.concatenate([jnp.concatenate([kv_s[b, 0], kv_s[b, 1]], axis=1) for b in blocks], axis=0)
        values = jnp.concatenate([jnp.concatenate([kv_s[b, 2], kv_s[b, 3]], axis=0) for b in blocks], axis=1)
        values = jnp.concatenate([values, jnp.ones((8, values.shape[1]), BF16)], axis=0)
        if masked:
            ok = lax.broadcasted_iota(jnp.int32, (both, both), 1) >= lax.broadcasted_iota(jnp.int32, (both, both), 0)

        def weigh(h, s):
            if masked:
                s = jnp.where(ok, s, HIDDEN)
            old = top_s[h]
            top = jnp.maximum(old, s.max(axis=0, keepdims=True))
            top_s[h] = top
            return h, jnp.exp2((s - top) * e).astype(BF16), jnp.exp2((old - top) * e)

        def mix(h, weights, keep):
            mix_s[h] = mix_s[h] * keep + dot(values, weights)

        scored, weighed = [], []
        for h in range(heads + AHEAD + BEHIND):
            if h < heads:
                scored.append((h, dot(keys, q_s[h])))
            if AHEAD <= h < heads + AHEAD:
                weighed.append(weigh(*scored.pop(0)))
            if AHEAD + BEHIND <= h:
                mix(*weighed.pop(0))

    def chip_blocks(r, c):
        return [device(r, c, 0), device(r, c, 1)]

    def row_blocks(r, k):
        return [device(r, along_row(d), k) for d in near]

    def wait_mate(blocks):
        for b in blocks:
            arrived(b)

    scope("near", lambda: second_0(start, True, last))
    scope("beside", lambda: beside(col - 1, start, True))
    scope("mate", lambda: arrived(mate))
    scope("diagonal", lambda: attend(chip_blocks(row, col), True))

    def own_row(t):
        c = col - 1 - t
        scope("above", lambda: above(t, start, True))
        scope("beside", lambda: beside(c - 1, start, True))
        scope("other", lambda: arrived(device(row, c, 1 - core)))
        scope("near", lambda: attend(chip_blocks(row, c)))

    many(col, own_row)
    scope("above", lambda: many(jnp.maximum(row - col, 0), lambda t: above(col + t, start, True)))

    def own_column(t):
        scope("other", lambda: arrived(device(earlier(t), col, 1 - core)))
        scope("column", lambda: attend(chip_blocks(earlier(t), col)))

    @pl.when(jnp.logical_not(last))
    def _():
        many(row, own_column)

        @pl.when(row > 0)
        def _():
            scope("third", lambda: third(earlier(0), start, True))

    @pl.when(last)
    def _():
        rows = [earlier(t) for t in range(side - 1)]
        scope("other", lambda: wait_mate([device(r, col, 1 - core) for r in rows]))
        scope("column", lambda: attend([b for r in rows for b in chip_blocks(r, col)]))
        scope("third", lambda: third(rows[0], start, True))

    def earlier_row(t):
        r = earlier(t)

        @pl.when(t + 1 < row)
        def _():
            scope("third", lambda: third(earlier(t + 1), start, True))

        scope("other", lambda: wait_mate(row_blocks(r, 1 - core)))
        scope("attend", lambda: attend(row_blocks(r, 0) + row_blocks(r, 1)))

    many(row, earlier_row)

    def give_o(s):
        at = pl.ds(pl.multiple_of(s * CHUNK, CHUNK), CHUNK)
        return remote(o_s.at[core, :, at], o_s.at[core, :, at], o_sem.at[0, s], o_sem.at[1, s], mate)

    def finish(s):
        for h in range(per):
            i = s * per + h
            whole = mix_s[i, :HEAD, :] * (1 / mix_s[i, HEAD : HEAD + 1, :])
            o_s[core, :, pl.ds(pl.multiple_of(s * CHUNK + h * HEAD, HEAD), HEAD)] = whole.T.astype(BF16)
        give_o(s).start()

    scope("finish", lambda: many(chunks, finish))

    for j in range(chunks):
        for k in range(2):
            load_wo(j, k).wait()

    def own_part(j):
        acc_s[j] = dot(o_s[core], wo_s[j, core])

    def take_o():
        for s in range(chunks):
            at = pl.ds(s * CHUNK, CHUNK)
            remote(o_s.at[1 - core, :, at], o_s.at[1 - core, :, at], o_sem.at[0, s], o_sem.at[1, s], mate).wait_recv()

    scope("own_part", lambda: many(chunks, own_part, chunks))
    scope("o_take", take_o)

    def give_y(j, there):
        at = pl.ds(pl.multiple_of(there * half + j * CHUNK, CHUNK), CHUNK)
        return remote(y_s.at[j], out_ref.at[:, at], y_sem.at[0, j], y_sem.at[1, j], mate)

    def tokens_of(k):
        return pl.ds(pl.multiple_of(k * own, own), own)

    def finished(j, k):
        at = pl.ds(pl.multiple_of(mine + j * CHUNK, CHUNK), CHUNK)
        more = dot(o_s[1 - core, tokens_of(k), :], wo_s[j, 1 - core])
        return at, (x_s[k, :, at].astype(F32) + (acc_s[j, tokens_of(k), :] + more)).astype(BF16)

    def give(j):
        y_s[j] = finished(j, 1 - core)[1]
        give_y(j, core).start()

    def keep(j):
        at, y = finished(j, core)
        out_ref[:, at] = y

    scope("give", lambda: many(chunks, give, chunks))
    scope("keep", lambda: many(chunks, keep, chunks))

    ending = jax.named_scope("ending")
    ending.__enter__()
    give_x.wait_send()
    first(sent)
    own_later(sent, True)
    second_0(sent, False, jnp.logical_not(last))
    second_1(sent, False)
    second_0(sent, False, last)
    many(row, lambda t: above(t, sent, False))
    many(col, lambda t: beside(t, sent, False))
    many(row, lambda t: third(t, sent, False))
    for j in range(chunks):
        give_o(j).wait_send()
        give_y(j, core).wait_send()
        give_y(j, 1 - core).wait_recv()
    ending.__exit__(None, None, None)


def angles(places):
    freq = THETA ** (-np.arange(HALF, dtype=np.float64) / HALF)
    a = np.asarray(places, np.float64)[:, None] * freq
    return np.stack([np.cos(a), np.sin(a)]).astype(np.float32)


def solution(mesh):
    n = mesh.shape["sp"]

    def step(x, gain, wq, wk, wv, wo):
        own, depth = x.shape
        both, half = 2 * own, depth // 2
        chunks = half // CHUNK
        heads = half // HEAD
        side = math.isqrt(n // 2)
        rel = angles(np.arange(both))
        base = angles(np.arange(n // 2) * both).transpose(1, 0, 2)
        base = np.pad(base, ((0, 0), (0, 6), (0, 0)))
        dma = pltpu.SemaphoreType.DMA
        hbm = pl.BlockSpec(memory_space=pltpu.HBM)
        return pl.pallas_call(
            functools.partial(kernel, n, own, depth),
            out_shape=pltpu.VMEM(x.shape, x.dtype),
            in_specs=[hbm] * 8,
            out_specs=pl.BlockSpec(memory_space=pltpu.VMEM),
            scratch_shapes=[
                pltpu.VMEM((2, own, depth), BF16),
                pltpu.VMEM((2, own, depth), BF16),
                pltpu.VMEM((depth,), BF16),
                pltpu.VMEM((depth, HEAD), BF16),
                pltpu.VMEM((depth, HEAD), BF16),
                pltpu.VMEM((chunks, depth, CHUNK), BF16),
                pltpu.VMEM((chunks, 2, half, CHUNK), BF16),
                pltpu.VMEM((2, both, HALF), F32),
                pltpu.VMEM((8, HALF), F32),
                pltpu.VMEM((both, HALF), F32),
                pltpu.VMEM((both, HALF), F32),
                pltpu.VMEM((n, 4, own, HALF), BF16),
                pltpu.VMEM((2, both, CHUNK), BF16),
                pltpu.VMEM((heads, HEAD, both), BF16),
                pltpu.VMEM((heads, 1, both), F32),
                pltpu.VMEM((heads, HEAD + 8, both), F32),
                pltpu.VMEM((2, both, half), BF16),
                pltpu.VMEM((chunks, both, CHUNK), F32),
                pltpu.VMEM((chunks, own, CHUNK), BF16),
                dma((6,)),
                dma((chunks,)),
                dma((chunks, 2)),
                dma((n,)),
                dma((2 * side - 1 + side * side + side * side,)),
                dma((2,)),
                dma((2, chunks)),
                dma((2, chunks)),
                pltpu.SemaphoreType.REGULAR,
                pltpu.SemaphoreType.REGULAR,
            ],
            compiler_params=pltpu.CompilerParams(collective_id=0, has_side_effects=True, vmem_limit_bytes=VMEM),
        )(x, gain, wq, wk, wv, wo, jnp.asarray(rel), jnp.asarray(base))

    tokens, whole = P(("dp", "sp"), None), P(None, None)
    return jax.shard_map(
        step,
        mesh=mesh,
        in_specs=(tokens, P(None), whole, whole, whole, whole),
        out_specs=tokens,
        check_vma=False,
    )
```

```python
import functools
import math

import jax
import jax.numpy as jnp
import numpy as np
from jax import lax
from jax.experimental import pallas as pl
from jax.experimental.pallas import tpu as pltpu
from jax.sharding import PartitionSpec as P

HEAD = 256
HALF = HEAD // 2
THETA = 10000
EPS = 1e-6
NEG = -1e30
HIDDEN = 2 * NEG
SCALE = HEAD**-0.5
LOG2E = 1.4426950408889634
AHEAD = 2
BEHIND = 2
VMEM = 62 * 2**20
PASS = 3, 2
CHUNK = 512
ROWS = 16
PARTS = 2
GIVEN = 2
F32, BF16 = jnp.float32, jnp.bfloat16


def dot(a, b, ca=1, cb=0):
    return lax.dot_general(a, b, (((ca,), (cb,)), ((), ())), preferred_element_type=F32)


def scope(name, f):
    with jax.named_scope(name):
        return f()


def many(n, f, unroll=1):
    lax.fori_loop(0, n, lambda i, _: (f(i), None)[1], None, unroll=unroll)


def kernel(n, own, depth, x_h, gain_h, wq_h, wk_h, wv_h, wo_h, rel_h, base_h, out_ref,
           x_s, xn_s, gain_s, wk_s, wv_s, wq_s, wo_s, rel_s, base_s, cos_s, sin_s, kv_s, raw_s, q_s, top_s, mix_s, o_s, acc_s, y_s,
           load_sem, wq_sem, wo_sem, recv_sem, send_sem, x_sem, o_sem, y_sem, meet, go):
    side = math.isqrt(n // 2)
    both = 2 * own
    me = lax.axis_index("sp")
    core, chip = lax.rem(me, 2), lax.div(me, 2)
    row, col = lax.div(chip, side), lax.rem(chip, side)
    mate = me + 1 - 2 * core
    half = depth // 2
    chunks = half // CHUNK
    per = CHUNK // HEAD
    heads = half // HEAD

    def device(r, c, k):
        return (r * side + c) * 2 + k

    def along_row(d):
        return lax.rem(col + d, side)

    def load(src, dst, i):
        return pltpu.make_async_copy(src, dst, load_sem.at[i])

    load_x = load(x_h, x_s.at[core], 0)
    load_gain = load(gain_h, gain_s, 1)
    load_wk = load(wk_h, wk_s, 2)
    load_wv = load(wv_h, wv_s, 3)
    load_rel = load(rel_h, rel_s, 4)
    load_base = load(base_h.at[chip], base_s, 5)
    mine = pl.multiple_of(core * half, CHUNK)

    def load_wq(j):
        return pltpu.make_async_copy(wq_h.at[:, pl.ds(pl.multiple_of(mine + j * CHUNK, CHUNK), CHUNK)], wq_s.at[j], wq_sem.at[j])

    def load_wo(j, k):
        return pltpu.make_async_copy(
            wo_h.at[pl.ds(k * half, half), pl.ds(pl.multiple_of(mine + j * CHUNK, CHUNK), CHUNK)], wo_s.at[j, k], wo_sem.at[j, k])

    for c in (load_x, load_gain, load_base, load_rel, load_wk, load_wv):
        c.start()

    barrier = pltpu.get_barrier_semaphore()
    peers = [device(row, along_row(d), 1) for d in range(1, side)] + [device(lax.rem(row + d, side), col, 1) for d in range(1, side)]

    def tell(sem, to):
        pl.semaphore_signal(sem, inc=1, device_id={"sp": to}, device_id_type=pl.DeviceIdType.MESH)

    def greet():
        @pl.when(core == 1)
        def _():
            tell(barrier, mate)

        @pl.when(core == 0)
        def _():
            pl.semaphore_wait(barrier, 1)
            tell(meet, mate)

        @pl.when(core == 1)
        def _():
            pl.semaphore_wait(meet, 1)
            for p in peers:
                tell(barrier, p)

    def gather():
        @pl.when(core == 1)
        def _():
            pl.semaphore_wait(barrier, len(peers))
            tell(go, mate)

        @pl.when(core == 0)
        def _():
            pl.semaphore_wait(go, 1)

    scope("greet", greet)

    def remote(src, dst, send, recv, to):
        return pltpu.make_async_remote_copy(src_ref=src, dst_ref=dst, send_sem=send, recv_sem=recv, device_id={"sp": to},
                                            device_id_type=pl.DeviceIdType.MESH)

    def block(b, to, i):
        return remote(kv_s.at[b], kv_s.at[b], send_sem.at[i], recv_sem.at[b], to)

    def arrived(b):
        block(b, mate, 0).wait_recv()

    def move_x(h, i):
        part = x_s.at[h, pl.ds(i * (own // PARTS), own // PARTS)]
        return remote(part, part, x_sem.at[0, i], x_sem.at[1, i], mate)


    load_base.wait()
    load_rel.wait()
    bc, bs = base_s[0:1, :], base_s[1:2, :]
    rc, rs = rel_s[0], rel_s[1]
    cos_s[...] = bc * rc - bs * rs
    sin_s[...] = bs * rc + bc * rs
    scope("x_wait", load_x.wait)
    for i in range(PARTS):
        move_x(core, i).start()
    load_gain.wait()

    gain = gain_s[...].astype(F32).reshape(1, depth)

    def norm(h, first, last):
        def some(i):
            i += first // ROWS
            at = pl.ds(pl.multiple_of(i * ROWS, ROWS), ROWS)
            wide = x_s[h, at, :].astype(F32)
            scale = lax.rsqrt(jnp.mean(wide * wide, -1, keepdims=True) + EPS)
            xn_s[h, at, :] = (wide * scale * gain).astype(BF16)

        many((last - first) // ROWS, some, 4)

    def turned(t, cos, sin):
        a, b = t[:, :HALF].astype(F32), t[:, HALF:].astype(F32)
        return (a * cos - b * sin).astype(BF16), (b * cos + a * sin).astype(BF16)

    scope("norm_own", lambda: norm(core, 0, own))
    for j in range(chunks):
        load_wq(j).start()
    at = pl.ds(pl.multiple_of(core * own, own), own)
    scope("wk_wait", load_wk.wait)
    ka, kb = turned(dot(xn_s[core], wk_s[...]).astype(BF16), cos_s[at, :], sin_s[at, :])
    kv_s[me, 0] = ka
    kv_s[me, 1] = kb
    scope("wv_wait", load_wv.wait)
    v = dot(xn_s[core], wv_s[...]).astype(BF16).T
    kv_s[me, 2] = v[:HALF]
    kv_s[me, 3] = v[HALF:]

    SECOND = 2 * side - 1
    THIRD = SECOND + side * side
    last = row == side - 1
    near = [1, side - 1, *range(2, side - 1)]

    def to_row(b, i, act, needs=None):
        for d in near:
            to = along_row(d)
            if needs is None:
                act(block(b, device(row, to, core), i + d - 1))
            else:
                @pl.when(needs(to))
                def _():
                    act(block(b, device(row, to, core), i + d - 1))

    def to_column(b, i, act):
        for d in (*range(2, side - 1), side - 1, 1):
            @pl.when(row + d < side)
            def _():
                act(block(b, device(row + d, col, core), i + d - 1))

    def first(act):
        @pl.when(core == 0)
        def _():
            to_row(me, 0, act, lambda c: jnp.logical_not(last) | (c > col))

        to_column(me, side - 1, act)
        act(block(me, mate, 2 * side - 2))

    def own_later(act, now):
        @pl.when((core == 1) & now)
        def _():
            to_row(me, 0, act, lambda c: c > col)

    def second_0(act, wait, now):
        for c in [jnp.where(last, i, along_row(d)) for i, d in zip((0, 1, 2), near)]:
            @pl.when((core == 0) & now & (c != col) & (jnp.logical_not(last) | (c < col)))
            def _():
                b, at = device(row, c, 0), SECOND + c * side
                if wait:
                    arrived(b)
                to_column(b, at, act)

                @pl.when(c < col)
                def _():
                    act(block(b, mate, at + side - 1))

    def second_1(act, wait):
        for t in range(side - 1):
            @pl.when((core == 1) & (t < row))
            def _():
                r = earlier(t)
                b, at = device(r, col, 1), SECOND + r * side
                if wait:
                    arrived(b)
                to_row(b, at, act)
                act(block(b, mate, at + side - 1))

    def beside(c, act, wait):
        @pl.when((core == 1) & (c >= 0))
        def _():
            b = device(row, c, 1)
            if wait:
                arrived(b)
            act(block(b, mate, THIRD + c))

    def above(t, act, wait):
        @pl.when((core == 0) & (t < row))
        def _():
            b = device(earlier(t), col, 0)
            if wait:
                arrived(b)
            act(block(b, mate, THIRD + (earlier(t) + 1) * side))

    def earlier(t):
        return jnp.where(last, row - 1 - t, t)

    def third(r, act, wait):
        at = THIRD + (r + 1) * side

        for d in near:
            b = device(r, along_row(d), core)
            if wait:
                arrived(b)

            act(block(b, mate, at + d))

    start = lambda c: c.start()
    sent = lambda c: c.wait_send()
    scope("gather", gather)
    scope("first", lambda: first(start))
    own_later(start, last)

    for i in range(PARTS):
        scope("x_take", move_x(1 - core, i).wait_recv)
        scope("norm_mate", lambda: norm(1 - core, i * (own // PARTS), (i + 1) * (own // PARTS)))

    def turn(j):
        for h in range(per):
            a, b = turned(raw_s[j % 2, :, h * HEAD : (h + 1) * HEAD], cos_s[...], sin_s[...])
            q_s[j * per + h, :HALF] = a.T
            q_s[j * per + h, HALF:] = b.T

    for j in range(chunks):
        for k in range(2):
            load_wo(j, k).start()
    for j in range(chunks):
        scope("wq_wait", load_wq(j).wait)
        with jax.named_scope("queries"):
            raw_s[j % 2] = dot(xn_s[...].reshape(both, depth), wq_s[j]).astype(BF16)
            if j:
                turn(j - 1)
        if j == 0:
            own_later(start, jnp.logical_not(last))
        if j == PASS[0]:
            scope("second", lambda: second_0(start, True, jnp.logical_not(last)))
        if j == PASS[1]:
            scope("second", lambda: second_1(start, True))
    scope("turn", lambda: turn(chunks - 1))

    e = SCALE * LOG2E
    for h in range(heads):
        top_s[h] = jnp.full((1, both), NEG, F32)
        mix_s[h] = jnp.zeros((HEAD + 8, both), F32)

    def attend(blocks, masked=False):
        keys = jnp.concatenate([jnp.concatenate([kv_s[b, 0], kv_s[b, 1]], axis=1) for b in blocks], axis=0)
        values = jnp.concatenate([jnp.concatenate([kv_s[b, 2], kv_s[b, 3]], axis=0) for b in blocks], axis=1)
        values = jnp.concatenate([values, jnp.ones((8, values.shape[1]), BF16)], axis=0)
        if masked:
            ok = lax.broadcasted_iota(jnp.int32, (both, both), 1) >= lax.broadcasted_iota(jnp.int32, (both, both), 0)

        def weigh(h, s):
            if masked:
                s = jnp.where(ok, s, HIDDEN)
            old = top_s[h]
            top = jnp.maximum(old, s.max(axis=0, keepdims=True))
            top_s[h] = top
            return h, jnp.exp2((s - top) * e).astype(BF16), jnp.exp2((old - top) * e)

        def mix(h, weights, keep):
            mix_s[h] = mix_s[h] * keep + dot(values, weights)

        scored, weighed = [], []
        for h in range(heads + AHEAD + BEHIND):
            if h < heads:
                scored.append((h, dot(keys, q_s[h])))
            if AHEAD <= h < heads + AHEAD:
                weighed.append(weigh(*scored.pop(0)))
            if AHEAD + BEHIND <= h:
                mix(*weighed.pop(0))

    def chip_blocks(r, c):
        return [device(r, c, 0), device(r, c, 1)]

    def row_blocks(r, k):
        return [device(r, along_row(d), k) for d in near]

    def wait_mate(blocks):
        for b in blocks:
            arrived(b)

    scope("near", lambda: second_0(start, True, last))
    scope("beside", lambda: beside(col - 1, start, True))
    scope("mate", lambda: arrived(mate))
    scope("diagonal", lambda: attend(chip_blocks(row, col), True))

    def own_row(t):
        c = col - 1 - t
        scope("above", lambda: above(t, start, True))
        scope("beside", lambda: beside(c - 1, start, True))
        scope("other", lambda: arrived(device(row, c, 1 - core)))
        scope("near", lambda: attend(chip_blocks(row, c)))

    corner = last & (col == side - 1)
    singles = jnp.where(corner, 0, col)
    many(singles, own_row)
    scope("above", lambda: many(jnp.maximum(row - singles, 0), lambda t: above(singles + t, start, True)))

    def own_column(t):
        scope("other", lambda: arrived(device(earlier(t), col, 1 - core)))
        scope("column", lambda: attend(chip_blocks(earlier(t), col)))

    @pl.when(jnp.logical_not(last))
    def _():
        many(row, own_column)

        @pl.when(row > 0)
        def _():
            scope("third", lambda: third(earlier(0), start, True))

    def line(k):
        places = [(jnp.where(k == 0, earlier(i), row), jnp.where(k == 0, col, i)) for i in range(side - 1)]
        scope("other", lambda: wait_mate([device(r, c, 1 - core) for r, c in places]))
        scope("column", lambda: attend([b for r, c in places for b in chip_blocks(r, c)]))

        @pl.when(k == 0)
        def _():
            @pl.when(corner)
            def _():
                scope("beside", lambda: many(col - 1, lambda c: beside(c, start, True)))

            scope("third", lambda: third(earlier(0), start, True))

    @pl.when(last)
    def _():
        many(jnp.where(corner, 2, 1), line)

    def earlier_row(t):
        r = earlier(t)

        @pl.when(t + 1 < row)
        def _():
            scope("third", lambda: third(earlier(t + 1), start, True))

        scope("other", lambda: wait_mate(row_blocks(r, 1 - core)))
        scope("attend", lambda: attend(row_blocks(r, 0) + row_blocks(r, 1)))

    many(row, earlier_row)

    def give_o(s):
        at = pl.ds(pl.multiple_of(s * CHUNK, CHUNK), CHUNK)
        return remote(o_s.at[core, :, at], o_s.at[core, :, at], o_sem.at[0, s], o_sem.at[1, s], mate)

    def finish(s):
        for h in range(per):
            i = s * per + h
            whole = mix_s[i, :HEAD, :] * (1 / mix_s[i, HEAD : HEAD + 1, :])
            o_s[core, :, pl.ds(pl.multiple_of(s * CHUNK + h * HEAD, HEAD), HEAD)] = whole.T.astype(BF16)
        give_o(s).start()

    scope("finish", lambda: many(chunks, finish))

    for j in range(chunks):
        for k in range(2):
            load_wo(j, k).wait()

    def own_part(j):
        acc_s[j] = dot(o_s[core], wo_s[j, core])

    def take_o():
        for s in range(chunks):
            at = pl.ds(s * CHUNK, CHUNK)
            remote(o_s.at[1 - core, :, at], o_s.at[1 - core, :, at], o_sem.at[0, s], o_sem.at[1, s], mate).wait_recv()

    scope("own_part", lambda: many(chunks, own_part, chunks))
    scope("o_take", take_o)

    def give_y(j, there):
        at = pl.ds(pl.multiple_of(there * half + j * GIVEN * CHUNK, CHUNK), GIVEN * CHUNK)
        return remote(y_s.at[j], out_ref.at[:, at], y_sem.at[0, j], y_sem.at[1, j], mate)

    def tokens_of(k):
        return pl.ds(pl.multiple_of(k * own, own), own)

    def finished(j, k):
        at = pl.ds(pl.multiple_of(mine + j * CHUNK, CHUNK), CHUNK)
        more = dot(o_s[1 - core, tokens_of(k), :], wo_s[j, 1 - core])
        return at, (x_s[k, :, at].astype(F32) + (acc_s[j, tokens_of(k), :] + more)).astype(BF16)

    def give(j):
        for i in range(GIVEN):
            y_s[j, :, i * CHUNK : (i + 1) * CHUNK] = finished(j * GIVEN + i, 1 - core)[1]
        give_y(j, core).start()

    def keep(j):
        at, y = finished(j, core)
        out_ref[:, at] = y

    scope("give", lambda: many(chunks // GIVEN, give, chunks // GIVEN))
    scope("keep", lambda: many(chunks, keep, chunks))

    ending = jax.named_scope("ending")
    ending.__enter__()
    for i in range(PARTS):
        move_x(core, i).wait_send()
    first(sent)
    own_later(sent, True)
    second_0(sent, False, jnp.logical_not(last))
    second_1(sent, False)
    second_0(sent, False, last)
    many(row, lambda t: above(t, sent, False))
    many(col, lambda t: beside(t, sent, False))
    many(row, lambda t: third(t, sent, False))
    for j in range(chunks):
        give_o(j).wait_send()
    for j in range(chunks // GIVEN):
        give_y(j, core).wait_send()
        give_y(j, 1 - core).wait_recv()
    ending.__exit__(None, None, None)


def angles(places):
    freq = THETA ** (-np.arange(HALF, dtype=np.float64) / HALF)
    a = np.asarray(places, np.float64)[:, None] * freq
    return np.stack([np.cos(a), np.sin(a)]).astype(np.float32)


def solution(mesh):
    n = mesh.shape["sp"]

    def step(x, gain, wq, wk, wv, wo):
        own, depth = x.shape
        both, half = 2 * own, depth // 2
        chunks = half // CHUNK
        heads = half // HEAD
        side = math.isqrt(n // 2)
        rel = angles(np.arange(both))
        base = angles(np.arange(n // 2) * both).transpose(1, 0, 2)
        base = np.pad(base, ((0, 0), (0, 6), (0, 0)))
        dma = pltpu.SemaphoreType.DMA
        hbm = pl.BlockSpec(memory_space=pltpu.HBM)
        return pl.pallas_call(
            functools.partial(kernel, n, own, depth),
            out_shape=pltpu.VMEM(x.shape, x.dtype),
            in_specs=[hbm] * 8,
            out_specs=pl.BlockSpec(memory_space=pltpu.VMEM),
            scratch_shapes=[
                pltpu.VMEM((2, own, depth), BF16),
                pltpu.VMEM((2, own, depth), BF16),
                pltpu.VMEM((depth,), BF16),
                pltpu.VMEM((depth, HEAD), BF16),
                pltpu.VMEM((depth, HEAD), BF16),
                pltpu.VMEM((chunks, depth, CHUNK), BF16),
                pltpu.VMEM((chunks, 2, half, CHUNK), BF16),
                pltpu.VMEM((2, both, HALF), F32),
                pltpu.VMEM((8, HALF), F32),
                pltpu.VMEM((both, HALF), F32),
                pltpu.VMEM((both, HALF), F32),
                pltpu.VMEM((n, 4, own, HALF), BF16),
                pltpu.VMEM((2, both, CHUNK), BF16),
                pltpu.VMEM((heads, HEAD, both), BF16),
                pltpu.VMEM((heads, 1, both), F32),
                pltpu.VMEM((heads, HEAD + 8, both), F32),
                pltpu.VMEM((2, both, half), BF16),
                pltpu.VMEM((chunks, both, CHUNK), F32),
                pltpu.VMEM((chunks // GIVEN, own, GIVEN * CHUNK), BF16),
                dma((6,)),
                dma((chunks,)),
                dma((chunks, 2)),
                dma((n,)),
                dma((2 * side - 1 + side * side + side * side,)),
                dma((2, PARTS)),
                dma((2, chunks)),
                dma((2, chunks // GIVEN)),
                pltpu.SemaphoreType.REGULAR,
                pltpu.SemaphoreType.REGULAR,
            ],
            compiler_params=pltpu.CompilerParams(collective_id=0, has_side_effects=True, vmem_limit_bytes=VMEM),
        )(x, gain, wq, wk, wv, wo, jnp.asarray(rel), jnp.asarray(base))

    tokens, whole = P(("dp", "sp"), None), P(None, None)
    return jax.shard_map(
        step,
        mesh=mesh,
        in_specs=(tokens, P(None), whole, whole, whole, whole),
        out_specs=tokens,
        check_vma=False,
    )
```

```python
import functools
import math

import jax
import jax.numpy as jnp
import numpy as np
from jax import lax
from jax.experimental import pallas as pl
from jax.experimental.pallas import tpu as pltpu
from jax.sharding import PartitionSpec as P

HEAD = 256
HALF = HEAD // 2
THETA = 10000
EPS = 1e-6
NEG = -1e30
HIDDEN = 2 * NEG
SCALE = HEAD**-0.5
LOG2E = 1.4426950408889634
AHEAD = 2
BEHIND = 2
VMEM = 62 * 2**20
PASS = 3, 2
CHUNK = 512
ROWS = 16
PARTS = 2
GIVEN = 2
F32, BF16 = jnp.float32, jnp.bfloat16


def dot(a, b, ca=1, cb=0):
    return lax.dot_general(a, b, (((ca,), (cb,)), ((), ())), preferred_element_type=F32)


def scope(name, f):
    with jax.named_scope(name):
        return f()


def many(n, f, unroll=1):
    lax.fori_loop(0, n, lambda i, _: (f(i), None)[1], None, unroll=unroll)


def kernel(n, own, depth, x_h, gain_h, wq_h, wk_h, wv_h, wo_h, rel_h, base_h, out_ref,
           x_s, xn_s, gain_s, wk_s, wv_s, wq_s, wo_s, rel_s, base_s, cos_s, sin_s, kv_s, raw_s, q_s, top_s, mix_s, o_s, acc_s, y_s,
           load_sem, wq_sem, wo_sem, recv_sem, send_sem, x_sem, o_sem, y_sem, meet, go):
    side = math.isqrt(n // 2)
    both = 2 * own
    me = lax.axis_index("sp")
    core, chip = lax.rem(me, 2), lax.div(me, 2)
    row, col = lax.div(chip, side), lax.rem(chip, side)
    mate = me + 1 - 2 * core
    half = depth // 2
    chunks = half // CHUNK
    per = CHUNK // HEAD
    heads = half // HEAD

    def device(r, c, k):
        return (r * side + c) * 2 + k

    def along_row(d):
        return lax.rem(col + d, side)

    def load(src, dst, i):
        return pltpu.make_async_copy(src, dst, load_sem.at[i])

    load_x = load(x_h, x_s.at[core], 0)
    load_gain = load(gain_h, gain_s, 1)
    load_wk = load(wk_h, wk_s, 2)
    load_wv = load(wv_h, wv_s, 3)
    load_rel = load(rel_h, rel_s, 4)
    load_base = load(base_h.at[chip], base_s, 5)
    mine = pl.multiple_of(core * half, CHUNK)

    def load_wq(j):
        return pltpu.make_async_copy(wq_h.at[:, pl.ds(pl.multiple_of(mine + j * CHUNK, CHUNK), CHUNK)], wq_s.at[j], wq_sem.at[j])

    def load_wo(j, k):
        return pltpu.make_async_copy(
            wo_h.at[pl.ds(k * half, half), pl.ds(pl.multiple_of(mine + j * CHUNK, CHUNK), CHUNK)], wo_s.at[j, k], wo_sem.at[j, k])

    for c in (load_x, load_gain, load_base, load_rel, load_wk, load_wv):
        c.start()

    barrier = pltpu.get_barrier_semaphore()
    peers = [device(row, along_row(d), 1) for d in range(1, side)] + [device(lax.rem(row + d, side), col, 1) for d in range(1, side)]

    def tell(sem, to):
        pl.semaphore_signal(sem, inc=1, device_id={"sp": to}, device_id_type=pl.DeviceIdType.MESH)

    def greet():
        @pl.when(core == 1)
        def _():
            tell(barrier, mate)

        @pl.when(core == 0)
        def _():
            pl.semaphore_wait(barrier, 1)
            tell(meet, mate)

        @pl.when(core == 1)
        def _():
            pl.semaphore_wait(meet, 1)
            for p in peers:
                tell(barrier, p)

    def gather():
        @pl.when(core == 1)
        def _():
            pl.semaphore_wait(barrier, len(peers))
            tell(go, mate)

        @pl.when(core == 0)
        def _():
            pl.semaphore_wait(go, 1)

    scope("greet", greet)

    def remote(src, dst, send, recv, to):
        return pltpu.make_async_remote_copy(src_ref=src, dst_ref=dst, send_sem=send, recv_sem=recv, device_id={"sp": to},
                                            device_id_type=pl.DeviceIdType.MESH)

    def block(b, to, i):
        return remote(kv_s.at[b], kv_s.at[b], send_sem.at[i], recv_sem.at[b], to)

    def arrived(b):
        block(b, mate, 0).wait_recv()

    def move_x(h, i):
        part = x_s.at[h, pl.ds(i * (own // PARTS), own // PARTS)]
        return remote(part, part, x_sem.at[0, i], x_sem.at[1, i], mate)


    load_base.wait()
    load_rel.wait()
    bc, bs = base_s[0:1, :], base_s[1:2, :]
    rc, rs = rel_s[0], rel_s[1]
    cos_s[...] = bc * rc - bs * rs
    sin_s[...] = bs * rc + bc * rs
    scope("x_wait", load_x.wait)
    for i in range(PARTS):
        move_x(core, i).start()
    load_gain.wait()

    gain = gain_s[...].astype(F32).reshape(1, depth)

    def norm(h, first, last):
        def some(i):
            i += first // ROWS
            at = pl.ds(pl.multiple_of(i * ROWS, ROWS), ROWS)
            wide = x_s[h, at, :].astype(F32)
            scale = lax.rsqrt(jnp.mean(wide * wide, -1, keepdims=True) + EPS)
            xn_s[h, at, :] = (wide * scale * gain).astype(BF16)

        many((last - first) // ROWS, some, 4)

    def turned(t, cos, sin):
        a, b = t[:, :HALF].astype(F32), t[:, HALF:].astype(F32)
        return (a * cos - b * sin).astype(BF16), (b * cos + a * sin).astype(BF16)

    scope("norm_own", lambda: norm(core, 0, own))
    for j in range(chunks):
        load_wq(j).start()
    at = pl.ds(pl.multiple_of(core * own, own), own)
    scope("wk_wait", load_wk.wait)
    ka, kb = turned(dot(xn_s[core], wk_s[...]).astype(BF16), cos_s[at, :], sin_s[at, :])
    kv_s[me, 0] = ka
    kv_s[me, 1] = kb
    scope("wv_wait", load_wv.wait)
    v = dot(xn_s[core], wv_s[...]).astype(BF16).T
    kv_s[me, 2] = v[:HALF]
    kv_s[me, 3] = v[HALF:]

    SECOND = 2 * side - 1
    THIRD = SECOND + side * side
    last = row == side - 1
    near = [1, side - 1, *range(2, side - 1)]

    def to_row(b, i, act, needs=None):
        for d in near:
            to = along_row(d)
            if needs is None:
                act(block(b, device(row, to, core), i + d - 1))
            else:
                @pl.when(needs(to))
                def _():
                    act(block(b, device(row, to, core), i + d - 1))

    def to_column(b, i, act):
        for d in (*range(2, side - 1), side - 1, 1):
            @pl.when(row + d < side)
            def _():
                act(block(b, device(row + d, col, core), i + d - 1))

    def first(act):
        @pl.when(core == 0)
        def _():
            to_row(me, 0, act, lambda c: jnp.logical_not(last) | (c > col))

        to_column(me, side - 1, act)
        act(block(me, mate, 2 * side - 2))

    def own_later(act, now):
        @pl.when((core == 1) & now)
        def _():
            to_row(me, 0, act, lambda c: c > col)

    def second_0(act, wait, now):
        for c in [jnp.where(last, i, along_row(d)) for i, d in zip((0, 1, 2), near)]:
            @pl.when((core == 0) & now & (c != col) & (jnp.logical_not(last) | (c < col)))
            def _():
                b, at = device(row, c, 0), SECOND + c * side
                if wait:
                    arrived(b)
                to_column(b, at, act)

                @pl.when(c < col)
                def _():
                    act(block(b, mate, at + side - 1))

    def second_1(act, wait):
        for t in range(side - 1):
            @pl.when((core == 1) & (t < row))
            def _():
                r = earlier(t)
                b, at = device(r, col, 1), SECOND + r * side
                if wait:
                    arrived(b)
                to_row(b, at, act)
                act(block(b, mate, at + side - 1))

    def beside(c, act, wait):
        @pl.when((core == 1) & (c >= 0))
        def _():
            b = device(row, c, 1)
            if wait:
                arrived(b)
            act(block(b, mate, THIRD + c))

    def above(t, act, wait):
        @pl.when((core == 0) & (t < row))
        def _():
            b = device(earlier(t), col, 0)
            if wait:
                arrived(b)
            act(block(b, mate, THIRD + (earlier(t) + 1) * side))

    def earlier(t):
        return jnp.where(last, row - 1 - t, t)

    def third(r, act, wait):
        at = THIRD + (r + 1) * side

        for d in near:
            b = device(r, along_row(d), core)
            if wait:
                arrived(b)

            act(block(b, mate, at + d))

    start = lambda c: c.start()
    sent = lambda c: c.wait_send()
    scope("gather", gather)
    scope("first", lambda: first(start))
    own_later(start, last)

    for i in range(PARTS):
        scope("x_take", move_x(1 - core, i).wait_recv)
        scope("norm_mate", lambda: norm(1 - core, i * (own // PARTS), (i + 1) * (own // PARTS)))

    def turn(j):
        for h in range(per):
            a, b = turned(raw_s[j % 2, :, h * HEAD : (h + 1) * HEAD], cos_s[...], sin_s[...])
            q_s[j * per + h, :HALF] = a.T
            q_s[j * per + h, HALF:] = b.T

    for j in range(chunks):
        for k in range(2):
            load_wo(j, k).start()
    for j in range(chunks):
        scope("wq_wait", load_wq(j).wait)
        with jax.named_scope("queries"):
            raw_s[j % 2] = dot(xn_s[...].reshape(both, depth), wq_s[j]).astype(BF16)
            if j:
                turn(j - 1)
        if j == 0:
            own_later(start, jnp.logical_not(last))
        if j == PASS[0]:
            scope("second", lambda: second_0(start, True, jnp.logical_not(last)))
        if j == PASS[1]:
            scope("second", lambda: second_1(start, True))
    scope("turn", lambda: turn(chunks - 1))

    e = SCALE * LOG2E
    for h in range(heads):
        top_s[h] = jnp.full((1, both), NEG, F32)
        mix_s[h] = jnp.zeros((HEAD + 8, both), F32)

    def attend(blocks, masked=False):
        keys = jnp.concatenate([jnp.concatenate([kv_s[b, 0], kv_s[b, 1]], axis=1) for b in blocks], axis=0)
        values = jnp.concatenate([jnp.concatenate([kv_s[b, 2], kv_s[b, 3]], axis=0) for b in blocks], axis=1)
        values = jnp.concatenate([values, jnp.ones((8, values.shape[1]), BF16)], axis=0)
        if masked:
            ok = lax.broadcasted_iota(jnp.int32, (both, both), 1) >= lax.broadcasted_iota(jnp.int32, (both, both), 0)

        def weigh(h, s):
            if masked:
                s = jnp.where(ok, s, HIDDEN)
            old = top_s[h]
            top = jnp.maximum(old, s.max(axis=0, keepdims=True))
            top_s[h] = top
            return h, jnp.exp2((s - top) * e).astype(BF16), jnp.exp2((old - top) * e)

        def mix(h, weights, keep):
            mix_s[h] = mix_s[h] * keep + dot(values, weights)

        scored, weighed = [], []
        for h in range(heads + AHEAD + BEHIND):
            if h < heads:
                scored.append((h, dot(keys, q_s[h])))
            if AHEAD <= h < heads + AHEAD:
                weighed.append(weigh(*scored.pop(0)))
            if AHEAD + BEHIND <= h:
                mix(*weighed.pop(0))

    def chip_blocks(r, c):
        return [device(r, c, 0), device(r, c, 1)]

    def row_blocks(r, k):
        return [device(r, along_row(d), k) for d in near]

    def wait_mate(blocks):
        for b in blocks:
            arrived(b)

    scope("beside", lambda: beside(col - 1, start, True))
    scope("mate", lambda: arrived(mate))
    scope("diagonal", lambda: attend(chip_blocks(row, col), True))
    scope("above", lambda: many(row, lambda t: above(t, start, True)))
    scope("near", lambda: second_0(start, True, last))

    def own_row(t):
        c = col - 1 - t
        scope("beside", lambda: beside(c - 1, start, True))
        scope("other", lambda: arrived(device(row, c, 1 - core)))
        scope("near", lambda: attend(chip_blocks(row, c)))

    corner = last & (col == side - 1)
    singles = jnp.where(corner, 0, col)
    many(singles, own_row)

    def own_column(t):
        scope("other", lambda: arrived(device(earlier(t), col, 1 - core)))
        scope("column", lambda: attend(chip_blocks(earlier(t), col)))

    @pl.when(jnp.logical_not(last))
    def _():
        many(row, own_column)

        @pl.when(row > 0)
        def _():
            scope("third", lambda: third(earlier(0), start, True))

    def line(k):
        places = [(jnp.where(k == 0, earlier(i), row), jnp.where(k == 0, col, i)) for i in range(side - 1)]

        @pl.when(corner & (k == 0))
        def _():
            scope("beside", lambda: many(col - 1, lambda c: beside(c, start, True)))

        ahead = (core == 1) & (col == side - 2)

        @pl.when(ahead)
        def _():
            scope("third", lambda: third(earlier(0), start, True))

        scope("other", lambda: wait_mate([device(r, c, 1 - core) for r, c in places]))
        scope("column", lambda: attend([b for r, c in places for b in chip_blocks(r, c)]))

        @pl.when(jnp.logical_not(ahead) & (k == jnp.where(corner & (core == 0), 1, 0)))
        def _():
            scope("third", lambda: third(earlier(0), start, True))

    @pl.when(last)
    def _():
        many(jnp.where(corner, 2, 1), line)

    def earlier_row(t):
        r = earlier(t)

        late = last & (col == 0) & (core == 1)
        split = late & (t == 0)

        def part(k):
            @pl.when(k == 1)
            def _():
                scope("other", lambda: wait_mate(row_blocks(r, 1 - core)))

            scope("part", lambda: attend(row_blocks(r, jnp.where(k == 0, core, 1 - core))))

        @pl.when(split)
        def _():
            many(2, part)

        @pl.when((t + 1 < row) & (jnp.logical_not(late) | split))
        def _():
            scope("third", lambda: third(earlier(t + 1), start, True))

        @pl.when(jnp.logical_not(split))
        def _():
            scope("other", lambda: wait_mate(row_blocks(r, 1 - core)))
            scope("attend", lambda: attend(row_blocks(r, 0) + row_blocks(r, 1)))

        @pl.when((t + 1 < row) & late & jnp.logical_not(split))
        def _():
            scope("third", lambda: third(earlier(t + 1), start, True))

    many(row, earlier_row)

    def give_o(s):
        at = pl.ds(pl.multiple_of(s * CHUNK, CHUNK), CHUNK)
        return remote(o_s.at[core, :, at], o_s.at[core, :, at], o_sem.at[0, s], o_sem.at[1, s], mate)

    def finish(s):
        for h in range(per):
            i = s * per + h
            whole = mix_s[i, :HEAD, :] * (1 / mix_s[i, HEAD : HEAD + 1, :])
            o_s[core, :, pl.ds(pl.multiple_of(s * CHUNK + h * HEAD, HEAD), HEAD)] = whole.T.astype(BF16)
        give_o(s).start()

    scope("finish", lambda: many(chunks, finish))

    for j in range(chunks):
        for k in range(2):
            load_wo(j, k).wait()

    def own_part(j):
        acc_s[j] = dot(o_s[core], wo_s[j, core])

    def take_o():
        for s in range(chunks):
            at = pl.ds(s * CHUNK, CHUNK)
            remote(o_s.at[1 - core, :, at], o_s.at[1 - core, :, at], o_sem.at[0, s], o_sem.at[1, s], mate).wait_recv()

    scope("own_part", lambda: many(chunks, own_part, chunks))
    scope("o_take", take_o)

    def give_y(j, there):
        at = pl.ds(pl.multiple_of(there * half + j * GIVEN * CHUNK, CHUNK), GIVEN * CHUNK)
        return remote(y_s.at[j], out_ref.at[:, at], y_sem.at[0, j], y_sem.at[1, j], mate)

    def tokens_of(k):
        return pl.ds(pl.multiple_of(k * own, own), own)

    def finished(j, k):
        at = pl.ds(pl.multiple_of(mine + j * CHUNK, CHUNK), CHUNK)
        more = dot(o_s[1 - core, tokens_of(k), :], wo_s[j, 1 - core])
        return at, (x_s[k, :, at].astype(F32) + (acc_s[j, tokens_of(k), :] + more)).astype(BF16)

    def give(j):
        for i in range(GIVEN):
            y_s[j, :, i * CHUNK : (i + 1) * CHUNK] = finished(j * GIVEN + i, 1 - core)[1]
        give_y(j, core).start()

    def keep(j):
        at, y = finished(j, core)
        out_ref[:, at] = y

    scope("give", lambda: many(chunks // GIVEN, give, chunks // GIVEN))
    scope("keep", lambda: many(chunks, keep, chunks))

    ending = jax.named_scope("ending")
    ending.__enter__()
    for i in range(PARTS):
        move_x(core, i).wait_send()
    first(sent)
    own_later(sent, True)
    second_0(sent, False, jnp.logical_not(last))
    second_1(sent, False)
    second_0(sent, False, last)
    many(row, lambda t: above(t, sent, False))
    many(col, lambda t: beside(t, sent, False))
    many(row, lambda t: third(t, sent, False))
    for j in range(chunks):
        give_o(j).wait_send()
    for j in range(chunks // GIVEN):
        give_y(j, core).wait_send()
        give_y(j, 1 - core).wait_recv()
    ending.__exit__(None, None, None)


def angles(places):
    freq = THETA ** (-np.arange(HALF, dtype=np.float64) / HALF)
    a = np.asarray(places, np.float64)[:, None] * freq
    return np.stack([np.cos(a), np.sin(a)]).astype(np.float32)


def solution(mesh):
    n = mesh.shape["sp"]

    def step(x, gain, wq, wk, wv, wo):
        own, depth = x.shape
        both, half = 2 * own, depth // 2
        chunks = half // CHUNK
        heads = half // HEAD
        side = math.isqrt(n // 2)
        rel = angles(np.arange(both))
        base = angles(np.arange(n // 2) * both).transpose(1, 0, 2)
        base = np.pad(base, ((0, 0), (0, 6), (0, 0)))
        dma = pltpu.SemaphoreType.DMA
        hbm = pl.BlockSpec(memory_space=pltpu.HBM)
        return pl.pallas_call(
            functools.partial(kernel, n, own, depth),
            out_shape=pltpu.VMEM(x.shape, x.dtype),
            in_specs=[hbm] * 8,
            out_specs=pl.BlockSpec(memory_space=pltpu.VMEM),
            scratch_shapes=[
                pltpu.VMEM((2, own, depth), BF16),
                pltpu.VMEM((2, own, depth), BF16),
                pltpu.VMEM((depth,), BF16),
                pltpu.VMEM((depth, HEAD), BF16),
                pltpu.VMEM((depth, HEAD), BF16),
                pltpu.VMEM((chunks, depth, CHUNK), BF16),
                pltpu.VMEM((chunks, 2, half, CHUNK), BF16),
                pltpu.VMEM((2, both, HALF), F32),
                pltpu.VMEM((8, HALF), F32),
                pltpu.VMEM((both, HALF), F32),
                pltpu.VMEM((both, HALF), F32),
                pltpu.VMEM((n, 4, own, HALF), BF16),
                pltpu.VMEM((2, both, CHUNK), BF16),
                pltpu.VMEM((heads, HEAD, both), BF16),
                pltpu.VMEM((heads, 1, both), F32),
                pltpu.VMEM((heads, HEAD + 8, both), F32),
                pltpu.VMEM((2, both, half), BF16),
                pltpu.VMEM((chunks, both, CHUNK), F32),
                pltpu.VMEM((chunks // GIVEN, own, GIVEN * CHUNK), BF16),
                dma((6,)),
                dma((chunks,)),
                dma((chunks, 2)),
                dma((n,)),
                dma((2 * side - 1 + side * side + side * side,)),
                dma((2, PARTS)),
                dma((2, chunks)),
                dma((2, chunks // GIVEN)),
                pltpu.SemaphoreType.REGULAR,
                pltpu.SemaphoreType.REGULAR,
            ],
            compiler_params=pltpu.CompilerParams(collective_id=0, has_side_effects=True, vmem_limit_bytes=VMEM),
        )(x, gain, wq, wk, wv, wo, jnp.asarray(rel), jnp.asarray(base))

    tokens, whole = P(("dp", "sp"), None), P(None, None)
    return jax.shard_map(
        step,
        mesh=mesh,
        in_specs=(tokens, P(None), whole, whole, whole, whole),
        out_specs=tokens,
        check_vma=False,
    )
```

```python
import functools
import math

import jax
import jax.numpy as jnp
import numpy as np
from jax import lax
from jax.experimental import pallas as pl
from jax.experimental.pallas import tpu as pltpu
from jax.sharding import PartitionSpec as P

HEAD = 256
HALF = HEAD // 2
THETA = 10000
EPS = 1e-6
NEG = -1e30
HIDDEN = 2 * NEG
SCALE = HEAD**-0.5
LOG2E = 1.4426950408889634
AHEAD = 2
BEHIND = 2
VMEM = 62 * 2**20
PASS = 3, 2
CHUNK = 512
ROWS = 16
PARTS = 2
GIVEN = 2
F32, BF16 = jnp.float32, jnp.bfloat16


def dot(a, b, ca=1, cb=0):
    return lax.dot_general(a, b, (((ca,), (cb,)), ((), ())), preferred_element_type=F32)


def scope(name, f):
    with jax.named_scope(name):
        return f()


def many(n, f, unroll=1):
    lax.fori_loop(0, n, lambda i, _: (f(i), None)[1], None, unroll=unroll)


def kernel(n, own, depth, x_h, gain_h, wq_h, wk_h, wv_h, wo_h, rel_h, base_h, out_ref,
           x_s, xn_s, gain_s, wk_s, wv_s, wq_s, wo_s, rel_s, base_s, cos_s, sin_s, kv_s, raw_s, q_s, top_s, mix_s, o_s, acc_s, y_s,
           load_sem, wq_sem, wo_sem, recv_sem, send_sem, x_sem, o_sem, y_sem, meet, go):
    side = math.isqrt(n // 2)
    both = 2 * own
    me = lax.axis_index("sp")
    core, chip = lax.rem(me, 2), lax.div(me, 2)
    row, col = lax.div(chip, side), lax.rem(chip, side)
    mate = me + 1 - 2 * core
    half = depth // 2
    chunks = half // CHUNK
    per = CHUNK // HEAD
    heads = half // HEAD

    def device(r, c, k):
        return (r * side + c) * 2 + k

    def along_row(d):
        return lax.rem(col + d, side)

    def load(src, dst, i):
        return pltpu.make_async_copy(src, dst, load_sem.at[i])

    load_x = load(x_h, x_s.at[core], 0)
    load_gain = load(gain_h, gain_s, 1)
    load_wk = load(wk_h, wk_s, 2)
    load_wv = load(wv_h, wv_s, 3)
    load_rel = load(rel_h, rel_s, 4)
    load_base = load(base_h.at[chip], base_s, 5)
    mine = pl.multiple_of(core * half, CHUNK)

    def load_wq(j):
        return pltpu.make_async_copy(wq_h.at[:, pl.ds(pl.multiple_of(mine + j * CHUNK, CHUNK), CHUNK)], wq_s.at[j], wq_sem.at[j])

    def load_wo(j, k):
        return pltpu.make_async_copy(
            wo_h.at[pl.ds(k * half, half), pl.ds(pl.multiple_of(mine + j * CHUNK, CHUNK), CHUNK)], wo_s.at[j, k], wo_sem.at[j, k])

    for c in (load_x, load_gain, load_base, load_rel, load_wk, load_wv):
        c.start()

    barrier = pltpu.get_barrier_semaphore()
    peers = [device(row, along_row(d), 1) for d in range(1, side)] + [device(lax.rem(row + d, side), col, 1) for d in range(1, side)]

    def tell(sem, to):
        pl.semaphore_signal(sem, inc=1, device_id={"sp": to}, device_id_type=pl.DeviceIdType.MESH)

    def greet():
        @pl.when(core == 1)
        def _():
            tell(barrier, mate)

        @pl.when(core == 0)
        def _():
            pl.semaphore_wait(barrier, 1)
            tell(meet, mate)

        @pl.when(core == 1)
        def _():
            pl.semaphore_wait(meet, 1)
            for p in peers:
                tell(barrier, p)

    def gather():
        @pl.when(core == 1)
        def _():
            pl.semaphore_wait(barrier, len(peers))
            tell(go, mate)

        @pl.when(core == 0)
        def _():
            pl.semaphore_wait(go, 1)

    scope("greet", greet)

    def remote(src, dst, send, recv, to):
        return pltpu.make_async_remote_copy(src_ref=src, dst_ref=dst, send_sem=send, recv_sem=recv, device_id={"sp": to},
                                            device_id_type=pl.DeviceIdType.MESH)

    def block(b, to, i):
        return remote(kv_s.at[b], kv_s.at[b], send_sem.at[i], recv_sem.at[b], to)

    def arrived(b):
        block(b, mate, 0).wait_recv()

    def move_x(h, i):
        part = x_s.at[h, pl.ds(i * (own // PARTS), own // PARTS)]
        return remote(part, part, x_sem.at[0, i], x_sem.at[1, i], mate)


    load_base.wait()
    load_rel.wait()
    bc, bs = base_s[0:1, :], base_s[1:2, :]
    rc, rs = rel_s[0], rel_s[1]
    cos_s[...] = bc * rc - bs * rs
    sin_s[...] = bs * rc + bc * rs
    scope("x_wait", load_x.wait)
    for i in range(PARTS):
        move_x(core, i).start()
    load_gain.wait()

    gain = gain_s[...].astype(F32).reshape(1, depth)

    def norm(h, first, last):
        def some(i):
            i += first // ROWS
            at = pl.ds(pl.multiple_of(i * ROWS, ROWS), ROWS)
            wide = x_s[h, at, :].astype(F32)
            scale = lax.rsqrt(jnp.mean(wide * wide, -1, keepdims=True) + EPS)
            xn_s[h, at, :] = (wide * scale * gain).astype(BF16)

        many((last - first) // ROWS, some, 4)

    def turned(t, cos, sin):
        a, b = t[:, :HALF].astype(F32), t[:, HALF:].astype(F32)
        return (a * cos - b * sin).astype(BF16), (b * cos + a * sin).astype(BF16)

    scope("norm_own", lambda: norm(core, 0, own))
    for j in range(chunks):
        load_wq(j).start()
    at = pl.ds(pl.multiple_of(core * own, own), own)
    scope("wk_wait", load_wk.wait)
    ka, kb = turned(dot(xn_s[core], wk_s[...]).astype(BF16), cos_s[at, :], sin_s[at, :])
    kv_s[me, 0] = ka
    kv_s[me, 1] = kb
    scope("wv_wait", load_wv.wait)
    v = dot(xn_s[core], wv_s[...]).astype(BF16).T
    kv_s[me, 2] = v[:HALF]
    kv_s[me, 3] = v[HALF:]

    SECOND = 2 * side - 1
    THIRD = SECOND + side * side
    last = row == side - 1
    near = [1, side - 1, *range(2, side - 1)]

    def to_row(b, i, act, needs=None):
        for d in near:
            to = along_row(d)
            if needs is None:
                act(block(b, device(row, to, core), i + d - 1))
            else:
                @pl.when(needs(to))
                def _():
                    act(block(b, device(row, to, core), i + d - 1))

    def to_column(b, i, act):
        for d in (*range(2, side - 1), side - 1, 1):
            @pl.when(row + d < side)
            def _():
                act(block(b, device(row + d, col, core), i + d - 1))

    def first(act):
        @pl.when(core == 0)
        def _():
            to_row(me, 0, act, lambda c: jnp.logical_not(last) | (c > col))

        to_column(me, side - 1, act)
        act(block(me, mate, 2 * side - 2))

    def own_later(act, now):
        @pl.when((core == 1) & now)
        def _():
            to_row(me, 0, act, lambda c: c > col)

    def second_0(act, wait, now):
        for c in [jnp.where(last, i, along_row(d)) for i, d in zip((0, 1, 2), near)]:
            @pl.when((core == 0) & now & (c != col) & (jnp.logical_not(last) | (c < col)))
            def _():
                b, at = device(row, c, 0), SECOND + c * side
                if wait:
                    arrived(b)
                to_column(b, at, act)

                @pl.when(c < col)
                def _():
                    act(block(b, mate, at + side - 1))

    def second_1(act, wait):
        for t in range(side - 1):
            @pl.when((core == 1) & (t < row))
            def _():
                r = earlier(t)
                b, at = device(r, col, 1), SECOND + r * side
                if wait:
                    arrived(b)
                to_row(b, at, act)
                act(block(b, mate, at + side - 1))

    def beside(c, act, wait):
        @pl.when((core == 1) & (c >= 0))
        def _():
            b = device(row, c, 1)
            if wait:
                arrived(b)
            act(block(b, mate, THIRD + c))

    def above(t, act, wait):
        @pl.when((core == 0) & (t < row))
        def _():
            b = device(earlier(t), col, 0)
            if wait:
                arrived(b)
            act(block(b, mate, THIRD + (earlier(t) + 1) * side))

    def earlier(t):
        return jnp.where(last, row - 1 - t, t)

    def third(r, act, wait):
        at = THIRD + (r + 1) * side

        for d in near:
            b = device(r, along_row(d), core)
            if wait:
                arrived(b)

            act(block(b, mate, at + d))

    start = lambda c: c.start()
    sent = lambda c: c.wait_send()
    scope("gather", gather)
    scope("first", lambda: first(start))
    own_later(start, last)

    for i in range(PARTS):
        scope("x_take", move_x(1 - core, i).wait_recv)
        scope("norm_mate", lambda: norm(1 - core, i * (own // PARTS), (i + 1) * (own // PARTS)))

    def turn(j):
        for h in range(per):
            a, b = turned(raw_s[j % 2, :, h * HEAD : (h + 1) * HEAD], cos_s[...], sin_s[...])
            q_s[j * per + h, :HALF] = a.T
            q_s[j * per + h, HALF:] = b.T

    for j in range(chunks):
        for k in range(2):
            load_wo(j, k).start()
    for j in range(chunks):
        scope("wq_wait", load_wq(j).wait)
        with jax.named_scope("queries"):
            raw_s[j % 2] = dot(xn_s[...].reshape(both, depth), wq_s[j]).astype(BF16)
            if j:
                turn(j - 1)
        if j == 0:
            own_later(start, jnp.logical_not(last))
        if j == PASS[0]:
            scope("second", lambda: second_0(start, True, jnp.logical_not(last)))
        if j == PASS[1]:
            scope("second", lambda: second_1(start, True))
    scope("turn", lambda: turn(chunks - 1))

    e = SCALE * LOG2E
    for h in range(heads):
        top_s[h] = jnp.full((1, both), NEG, F32)
        mix_s[h] = jnp.zeros((HEAD + 8, both), F32)

    def attend(blocks, masked=False):
        keys = jnp.concatenate([jnp.concatenate([kv_s[b, 0], kv_s[b, 1]], axis=1) for b in blocks], axis=0)
        values = jnp.concatenate([jnp.concatenate([kv_s[b, 2], kv_s[b, 3]], axis=0) for b in blocks], axis=1)
        values = jnp.concatenate([values, jnp.ones((8, values.shape[1]), BF16)], axis=0)
        if masked:
            ok = lax.broadcasted_iota(jnp.int32, (both, both), 1) >= lax.broadcasted_iota(jnp.int32, (both, both), 0)

        def weigh(h, s):
            if masked:
                s = jnp.where(ok, s, HIDDEN)
            old = top_s[h]
            top = jnp.maximum(old, s.max(axis=0, keepdims=True))
            top_s[h] = top
            return h, jnp.exp2((s - top) * e).astype(BF16), jnp.exp2((old - top) * e)

        def mix(h, weights, keep):
            mix_s[h] = mix_s[h] * keep + dot(values, weights)

        scored, weighed = [], []
        for h in range(heads + AHEAD + BEHIND):
            if h < heads:
                scored.append((h, dot(keys, q_s[h])))
            if AHEAD <= h < heads + AHEAD:
                weighed.append(weigh(*scored.pop(0)))
            if AHEAD + BEHIND <= h:
                mix(*weighed.pop(0))

    def chip_blocks(r, c):
        return [device(r, c, 0), device(r, c, 1)]

    def row_blocks(r, k):
        return [device(r, along_row(d), k) for d in near]

    def wait_mate(blocks):
        for b in blocks:
            arrived(b)

    scope("beside", lambda: beside(col - 1, start, True))
    scope("mate", lambda: arrived(mate))
    scope("diagonal", lambda: attend(chip_blocks(row, col), True))
    scope("above", lambda: many(row, lambda t: above(t, start, True)))
    scope("near", lambda: second_0(start, True, last))

    def own_row(t):
        c = col - 1 - t
        scope("beside", lambda: beside(c - 1, start, True))
        scope("other", lambda: arrived(device(row, c, 1 - core)))
        scope("near", lambda: attend(chip_blocks(row, c)))

    corner = last & (col == side - 1)
    singles = jnp.where(corner, 0, col)
    many(singles, own_row)

    def own_column(t):
        scope("other", lambda: arrived(device(earlier(t), col, 1 - core)))
        scope("column", lambda: attend(chip_blocks(earlier(t), col)))

    @pl.when(jnp.logical_not(last))
    def _():
        many(row, own_column)

        @pl.when(row > 0)
        def _():
            scope("third", lambda: third(earlier(0), start, True))

    def line(k):
        places = [(jnp.where(k == 0, earlier(i), row), jnp.where(k == 0, col, i)) for i in range(side - 1)]

        @pl.when(corner & (k == 0))
        def _():
            scope("beside", lambda: many(col - 1, lambda c: beside(c, start, True)))

        ahead = (core == 1) & (col == side - 2)

        @pl.when(ahead)
        def _():
            scope("third", lambda: third(earlier(0), start, True))

        scope("other", lambda: wait_mate([device(r, c, 1 - core) for r, c in places]))
        scope("column", lambda: attend([b for r, c in places for b in chip_blocks(r, c)]))

        @pl.when(jnp.logical_not(ahead) & (k == jnp.where(corner & (core == 0), 1, 0)))
        def _():
            scope("third", lambda: third(earlier(0), start, True))

    @pl.when(last)
    def _():
        many(jnp.where(corner, 2, 1), line)

    def earlier_row(t):
        r = earlier(t)

        late = last & (col == 0) & (core == 1)
        split = late & (t == 0)

        def part(k):
            @pl.when(k == 1)
            def _():
                scope("other", lambda: wait_mate(row_blocks(r, 1 - core)))

            scope("part", lambda: attend(row_blocks(r, jnp.where(k == 0, core, 1 - core))))

        @pl.when(split)
        def _():
            many(2, part)

        @pl.when((t + 1 < row) & (jnp.logical_not(late) | split))
        def _():
            scope("third", lambda: third(earlier(t + 1), start, True))

        @pl.when(jnp.logical_not(split))
        def _():
            scope("other", lambda: wait_mate(row_blocks(r, 1 - core)))
            scope("attend", lambda: attend(row_blocks(r, 0) + row_blocks(r, 1)))

        @pl.when((t + 1 < row) & late & jnp.logical_not(split))
        def _():
            scope("third", lambda: third(earlier(t + 1), start, True))

    many(row, earlier_row)

    def give_o(s):
        at = pl.ds(pl.multiple_of(s * CHUNK, CHUNK), CHUNK)
        return remote(o_s.at[core, :, at], o_s.at[core, :, at], o_sem.at[0, s], o_sem.at[1, s], mate)

    def finish(s):
        for h in range(per):
            i = s * per + h
            whole = mix_s[i, :HEAD, :] * (1 / mix_s[i, HEAD : HEAD + 1, :])
            o_s[core, :, pl.ds(pl.multiple_of(s * CHUNK + h * HEAD, HEAD), HEAD)] = whole.T.astype(BF16)
        give_o(s).start()

    scope("finish", lambda: many(chunks, finish, chunks))

    for j in range(chunks):
        for k in range(2):
            load_wo(j, k).wait()

    def own_part(j):
        acc_s[j] = dot(o_s[core], wo_s[j, core])

    def take_o():
        for s in range(chunks):
            at = pl.ds(s * CHUNK, CHUNK)
            remote(o_s.at[1 - core, :, at], o_s.at[1 - core, :, at], o_sem.at[0, s], o_sem.at[1, s], mate).wait_recv()

    scope("own_part", lambda: many(chunks, own_part, chunks))
    scope("o_take", take_o)

    def give_y(j, there):
        at = pl.ds(pl.multiple_of(there * half + j * GIVEN * CHUNK, CHUNK), GIVEN * CHUNK)
        return remote(y_s.at[j], out_ref.at[:, at], y_sem.at[0, j], y_sem.at[1, j], mate)

    def tokens_of(k):
        return pl.ds(pl.multiple_of(k * own, own), own)

    def finished(j, k):
        at = pl.ds(pl.multiple_of(mine + j * CHUNK, CHUNK), CHUNK)
        more = dot(o_s[1 - core, tokens_of(k), :], wo_s[j, 1 - core])
        return at, (x_s[k, :, at].astype(F32) + (acc_s[j, tokens_of(k), :] + more)).astype(BF16)

    def give(j):
        for i in range(GIVEN):
            y_s[j, :, i * CHUNK : (i + 1) * CHUNK] = finished(j * GIVEN + i, 1 - core)[1]
        give_y(j, core).start()

    def keep(j):
        at, y = finished(j, core)
        out_ref[:, at] = y

    scope("give", lambda: many(chunks // GIVEN, give, chunks // GIVEN))
    scope("keep", lambda: many(chunks, keep, chunks))

    ending = jax.named_scope("ending")
    ending.__enter__()
    for i in range(PARTS):
        move_x(core, i).wait_send()
    first(sent)
    own_later(sent, True)
    second_0(sent, False, jnp.logical_not(last))
    second_1(sent, False)
    second_0(sent, False, last)
    many(row, lambda t: above(t, sent, False))
    many(col, lambda t: beside(t, sent, False))
    many(row, lambda t: third(t, sent, False))
    for j in range(chunks):
        give_o(j).wait_send()
    for j in range(chunks // GIVEN):
        give_y(j, core).wait_send()
        give_y(j, 1 - core).wait_recv()
    ending.__exit__(None, None, None)


def angles(places):
    freq = THETA ** (-np.arange(HALF, dtype=np.float64) / HALF)
    a = np.asarray(places, np.float64)[:, None] * freq
    return np.stack([np.cos(a), np.sin(a)]).astype(np.float32)


def solution(mesh):
    n = mesh.shape["sp"]

    def step(x, gain, wq, wk, wv, wo):
        own, depth = x.shape
        both, half = 2 * own, depth // 2
        chunks = half // CHUNK
        heads = half // HEAD
        side = math.isqrt(n // 2)
        rel = angles(np.arange(both))
        base = angles(np.arange(n // 2) * both).transpose(1, 0, 2)
        base = np.pad(base, ((0, 0), (0, 6), (0, 0)))
        dma = pltpu.SemaphoreType.DMA
        hbm = pl.BlockSpec(memory_space=pltpu.HBM)
        return pl.pallas_call(
            functools.partial(kernel, n, own, depth),
            out_shape=pltpu.VMEM(x.shape, x.dtype),
            in_specs=[hbm] * 8,
            out_specs=pl.BlockSpec(memory_space=pltpu.VMEM),
            scratch_shapes=[
                pltpu.VMEM((2, own, depth), BF16),
                pltpu.VMEM((2, own, depth), BF16),
                pltpu.VMEM((depth,), BF16),
                pltpu.VMEM((depth, HEAD), BF16),
                pltpu.VMEM((depth, HEAD), BF16),
                pltpu.VMEM((chunks, depth, CHUNK), BF16),
                pltpu.VMEM((chunks, 2, half, CHUNK), BF16),
                pltpu.VMEM((2, both, HALF), F32),
                pltpu.VMEM((8, HALF), F32),
                pltpu.VMEM((both, HALF), F32),
                pltpu.VMEM((both, HALF), F32),
                pltpu.VMEM((n, 4, own, HALF), BF16),
                pltpu.VMEM((2, both, CHUNK), BF16),
                pltpu.VMEM((heads, HEAD, both), BF16),
                pltpu.VMEM((heads, 1, both), F32),
                pltpu.VMEM((heads, HEAD + 8, both), F32),
                pltpu.VMEM((2, both, half), BF16),
                pltpu.VMEM((chunks, both, CHUNK), F32),
                pltpu.VMEM((chunks // GIVEN, own, GIVEN * CHUNK), BF16),
                dma((6,)),
                dma((chunks,)),
                dma((chunks, 2)),
                dma((n,)),
                dma((2 * side - 1 + side * side + side * side,)),
                dma((2, PARTS)),
                dma((2, chunks)),
                dma((2, chunks // GIVEN)),
                pltpu.SemaphoreType.REGULAR,
                pltpu.SemaphoreType.REGULAR,
            ],
            compiler_params=pltpu.CompilerParams(collective_id=0, has_side_effects=True, vmem_limit_bytes=VMEM),
        )(x, gain, wq, wk, wv, wo, jnp.asarray(rel), jnp.asarray(base))

    tokens, whole = P(("dp", "sp"), None), P(None, None)
    return jax.shard_map(
        step,
        mesh=mesh,
        in_specs=(tokens, P(None), whole, whole, whole, whole),
        out_specs=tokens,
        check_vma=False,
    )
```
